128 devices in a mesh: section: 4 (over z), dp: 8 (over y, core), mp: 4 (over x).
Axes of the slice: x: 4, y: 4, z: 4, core: 2. Of those that a mesh axis runs over, the one named last changes fastest.
Arguments:
- text: bfloat16 [4, 4096, 4096], P('section', ('dp', 'mp')), may hold values from -6 to 6
- patches: bfloat16 [16384, 1024], P(('section', 'dp')), may hold values from -6 to 6
- segments: int32 [4, 8, 512], P('section', 'dp'), may hold values from 0 to 3, never falling along the last dimension, each value on 1 to 256 neighbouring positions
- loss_mask: int32 [4, 4096], P('section', ('dp', 'mp')), may hold values from 0 to 1, as said below
- tile_batch: int32 [8, 8], P('dp'), may hold values from 0 to 3, as said below
- tile_offset: int32 [8, 8], P('dp'), may hold values from 0 to 448, as said below
- attn_gain: float32 [4, 4096], P('section'), may hold values from 0.5 to 2
- w_query: bfloat16 [4, 4096, 2048], P('section', None, 'mp'), may hold values from -0.09375 to 0.09375
- w_kv: bfloat16 [4, 2, 4096, 512], P('section', None, None, 'mp'), may hold values from -0.09375 to 0.09375
- w_out: bfloat16 [4, 2048, 4096], P('section', 'mp'), may hold values from -0.125 to 0.125
- vis_gain: float32 [2, 1024], replicated, may hold values from 0.5 to 2
- vis_bias: float32 [2, 1024], replicated, may hold values from -3 to 3
- v_qkv: bfloat16 [3, 1024, 1024], P(None, ('section', 'dp'), 'mp'), may hold values from -0.1875 to 0.1875
- v_out: bfloat16 [1024, 1024], P('mp', ('section', 'dp')), may hold values from -0.1875 to 0.1875
- v_up: bfloat16 [1024, 4096], P(('section', 'dp'), 'mp'), may hold values from -0.1875 to 0.1875
- v_down: bfloat16 [4096, 1024], P('mp', ('section', 'dp')), may hold values from -0.09375 to 0.09375
- v_proj: bfloat16 [4096, 4096], P(('section', 'dp'), 'mp'), may hold values from -0.09375 to 0.09375
Outputs:
- hidden: bfloat16 [4, 4096, 4096], P('section', ('dp', 'mp'))
- token_weight: float32 [4, 4096], P('section', ('dp', 'mp'))
The draws below stay inside these ranges and needn't reach their ends.
Inputs may be any that keep to these rules, and one draw needn't show every extreme that they name: `tile_batch`: in every data-parallel index, the 2 tiles of each section index go 1 to each of two different micro-batches; one micro-batch receives 1 tiles from every section index. `tile_offset`: offsets are multiples of 64; the runs of one sequence never intersect. `loss_mask`: the first position of every sequence is a one.
All inputs are finite; a program needn't handle non-finite values.
Results may differ from the reference program's by a relative error of at most 0.025.
Values may be sent and summed in bfloat16 or wider, within the bound.
A program may use at most 192 MiB of HBM per device.

```python
import math
import jax
import jax.numpy as jnp
import numpy as np
from jax import lax

D = 4096
QH = 16
KVH = 4
HD = 128
VD = 1024
VH = 16
VHD = 64
VFF = 4096
GRID = 16
PATCH = 256
POOL = 64
L = 512
TILES_G = 2
CAP = 1
MICRO = 4
TILES = 64
N_SECTION = 4
N_DP = 8
N_MP = 4


def tile_plan(key):
    base_key = jax.random.fold_in(key, 7)
    target_key, second_key, order_key, slot_key = jax.random.split(base_key, 4)
    tile_count = N_SECTION * TILES_G
    target = jax.random.randint(target_key, (N_DP, 1), 0, MICRO)
    moved = jax.random.randint(second_key, (N_DP, N_SECTION), 1, MICRO)
    second = jnp.mod(target + moved, MICRO)
    orders = jax.vmap(lambda item_key: jax.random.permutation(item_key, TILES_G))(jax.random.split(order_key, N_DP * N_SECTION))
    orders = orders.reshape(N_DP, N_SECTION, TILES_G)
    batches = jnp.where(orders < CAP, target[:, :, None], second[:, :, None]).reshape(N_DP, tile_count)
    tile_ids = jnp.arange(tile_count, dtype=jnp.int32)
    earlier = tile_ids[None, :] < tile_ids[:, None]
    same = batches[:, :, None] == batches[:, None, :]
    ranks = jnp.sum((same & earlier[None, :, :]).astype(jnp.int32), axis=2)
    slot_total = L // POOL
    slot_perm = jax.vmap(lambda item_key: jax.random.permutation(item_key, slot_total))(jax.random.split(slot_key, N_DP * MICRO))
    slot_perm = slot_perm.reshape(N_DP, MICRO * slot_total)
    offsets = POOL * jnp.take_along_axis(slot_perm, batches * slot_total + ranks, axis=1)
    return (batches.astype(jnp.int32), offsets.astype(jnp.int32))


def draw_tile_batch(key, part):
    batches, offsets = tile_plan(key)
    return batches


def draw_tile_offset(key, part):
    batches, offsets = tile_plan(key)
    return offsets


def draw_loss_mask(key, part):
    seq_count = MICRO * N_DP
    seq_index = jnp.arange(seq_count, dtype=jnp.int32)
    threshold = 250 + 500 * seq_index // max(seq_count - 1, 1)
    rolls = jax.random.randint(jax.random.fold_in(key, 5), (seq_count, L), 0, 1000)
    marked = (rolls < threshold[:, None]).astype(jnp.int32)
    leading = (jnp.arange(L) == 0).astype(jnp.int32)
    marked = jnp.maximum(marked, leading[None, :])
    return marked.reshape(MICRO, N_DP * L)


def gain_values(key, shape):
    return jax.random.uniform(key, shape, jnp.float32, 0.5, 1.5)


def draw_attn_gain(key, part):
    return gain_values(jax.random.fold_in(key, 3), (N_SECTION, D))


def draw_vis_gain(key, part):
    return gain_values(jax.random.fold_in(key, 4), (2, VD))


def shard_levels(stream_key, extent, pieces, low, high):
    level, own = 1.0, jax.random.fold_in(stream_key, 6)
    for axis_at, shards_of in pieces:
        heights = jnp.exp(jax.random.uniform(jax.random.fold_in(own, axis_at), (shards_of,), jnp.float32, low / len(pieces), high / len(pieces)))
        level = level * jnp.repeat(heights, extent[axis_at] // shards_of).reshape([-1 if axis == axis_at else 1 for axis in range(len(extent))])
    return level


def split_up(number_of, total, bound, slope):
    loads = [(1 << 20) // math.isqrt(grade ** slope) + 1 for grade in range(2, number_of + 1)]
    surplus, given = total - bound - (number_of - 1), [1] * (number_of - 1)
    while surplus > 0:
        free = [i for i in range(number_of - 1) if given[i] < bound]
        pool, remaining = sum([loads[i] for i in free]), surplus
        for i in free:
            extra = min(bound - given[i], max(1, remaining * loads[i] // pool), surplus)
            given[i] = given[i] + extra
            surplus = surplus - extra
    return np.array([bound] + given)


def uneven(rng, count, total, reach, slope):
    if count == 2:
        one = jax.random.randint(rng, (), max(1, total - reach), min(reach, total - 1) + 1)
        return jnp.stack([one, total - one])
    sizes = jnp.asarray(split_up(count, total, reach, slope), jnp.int32)
    twos = (count - 1) // 2
    source_of, sink = sizes[1:1 + 2 * twos:2], sizes[2:2 + 2 * twos:2]
    margin = jnp.minimum(source_of - 1, reach - sink)
    shifted = jax.random.randint(jax.random.fold_in(rng, 1), (twos,), 0, 1 << 20) % (margin + 1)
    sizes = sizes.at[1:1 + 2 * twos:2].set(source_of - shifted).at[2:2 + 2 * twos:2].set(sink + shifted)
    return sizes[jax.random.permutation(jax.random.fold_in(rng, 2), count)]


def normal_values(stream_key, shape, scale, bound, pieces=(), kind=jnp.bfloat16):
    values = jax.random.normal(stream_key, shape, jnp.float32) * scale
    if len(pieces) > 0:
        values = shard_levels(stream_key, shape, pieces, -0.22, 0.18) * values
    return jnp.clip(values, min=-bound, max=bound).astype(kind)


def setup_inputs(seed: int = 0) -> dict:
    key_list = jax.random.split(jax.random.key(seed), 18)
    return {
        "text": normal_values(key_list[0], (MICRO, N_DP * L, D), 1.0, 6.0, ((0, 4), (1, 32))),
        "patches": normal_values(key_list[1], (TILES * PATCH, VD), 1.0, 6.0, ((0, 32),)),
        "segments": jax.vmap(lambda own: jnp.searchsorted(jnp.cumsum(uneven(own, 4, L, L // 2, 2)), jnp.arange(L), side="right"))(jax.random.split(key_list[2], MICRO * N_DP)).reshape((MICRO, N_DP, L)).astype(jnp.int32),
        "loss_mask": draw_loss_mask(jax.random.fold_in(key_list[17], 71), 0),
        "tile_batch": draw_tile_batch(jax.random.fold_in(key_list[17], 71), 0),
        "tile_offset": draw_tile_offset(jax.random.fold_in(key_list[17], 71), 0),
        "attn_gain": draw_attn_gain(jax.random.fold_in(key_list[17], 71), 0),
        "w_query": normal_values(key_list[7], (N_SECTION, D, QH * HD), D ** -0.5, 0.09375, ((0, 4), (2, 4))),
        "w_kv": normal_values(key_list[8], (N_SECTION, 2, D, KVH * HD), D ** -0.5, 0.09375, ((0, 4), (3, 4))),
        "w_out": normal_values(key_list[9], (N_SECTION, QH * HD, D), (QH * HD) ** -0.5, 0.125, ((0, 4), (1, 4))),
        "vis_gain": draw_vis_gain(jax.random.fold_in(key_list[17], 71), 0),
        "vis_bias": normal_values(key_list[11], (2, VD), 0.5, 3.0, (), jnp.float32),
        "v_qkv": normal_values(key_list[12], (3, VD, VD), VD ** -0.5, 0.1875, ((1, 32), (2, 4))),
        "v_out": normal_values(key_list[13], (VD, VD), VD ** -0.5, 0.1875, ((0, 4), (1, 32))),
        "v_up": normal_values(key_list[14], (VD, VFF), VD ** -0.5, 0.1875, ((0, 32), (1, 4))),
        "v_down": normal_values(key_list[15], (VFF, VD), VFF ** -0.5, 0.09375, ((0, 4), (1, 32))),
        "v_proj": normal_values(key_list[16], (4 * VD, D), (4 * VD) ** -0.5, 0.09375, ((0, 32), (1, 4))),
    }


EPS = 1e-05
ROPE_BASE = 500000.0
BLOCKED = -1e+30

def layer_norm(values, gain, bias):
    wide = values.astype(jnp.float32)
    center = wide - lax.optimization_barrier(jnp.mean(wide, axis=-1, keepdims=True))
    spread = lax.optimization_barrier(jnp.mean(center * center, axis=-1, keepdims=True))
    return (center * lax.rsqrt(spread + EPS) * gain + bias).astype(jnp.bfloat16)

def rms_norm(values, gain):
    wide = values.astype(jnp.float32)
    power = lax.optimization_barrier(jnp.mean(wide * wide, axis=-1, keepdims=True))
    return (wide * lax.rsqrt(power + EPS) * gain).astype(jnp.bfloat16)

def rotate(values, positions):
    half_width = values.shape[-1] // 2
    freqs = ROPE_BASE ** (-2.0 * jnp.arange(half_width, dtype=jnp.float32) / values.shape[-1])
    angles = positions.astype(jnp.float32)[:, None] * freqs[None, :]
    cosine = jnp.cos(angles)[:, None, :]
    sinus_part = jnp.sin(angles)[:, None, :]
    first_half = values[..., :half_width]
    second_half = values[..., half_width:]
    return jnp.concatenate([first_half * cosine - second_half * sinus_part, second_half * cosine + first_half * sinus_part], axis=-1)

def split_sum(left, right):
    row_count = left.shape[0]
    block_width = left.shape[1] // N_MP
    left_blocks = left.reshape(row_count, N_MP, block_width).astype(jnp.float32)
    right_blocks = right.reshape(N_MP, block_width, right.shape[1]).astype(jnp.float32)
    partials = jnp.einsum('rgk,gkn->grn', left_blocks, right_blocks)
    rounded = lax.optimization_barrier(partials.astype(jnp.bfloat16))
    return lax.optimization_barrier(jnp.sum(rounded.astype(jnp.float32), axis=0))

def pixel_shuffle(states):
    tile_count = states.shape[0] // PATCH
    side_half = GRID // 2
    width = states.shape[1]
    arranged = states.reshape(tile_count, side_half, 2, side_half, 2, width)
    return arranged.transpose(0, 1, 3, 2, 4, 5).reshape(tile_count * side_half * side_half, 4 * width)

def encode_group(block, vis_gain, vis_bias, v_qkv, v_out, v_up, v_down, v_proj):
    tile_count = block.shape[0] // PATCH
    normed = layer_norm(block, vis_gain[0], vis_bias[0])
    projected = [jnp.dot(normed, v_qkv[index], preferred_element_type=jnp.float32).astype(jnp.bfloat16).reshape(tile_count, PATCH, VH, VHD) for index in range(3)]
    scores = jnp.einsum('tqhd,tkhd->thqk', projected[0].astype(jnp.float32), projected[1].astype(jnp.float32)) * VHD ** (-0.5)
    probs = jax.nn.softmax(scores, axis=-1).astype(jnp.bfloat16)
    mixed = jnp.einsum('thqk,tkhd->tqhd', probs.astype(jnp.float32), projected[2].astype(jnp.float32)).astype(jnp.bfloat16).reshape(tile_count * PATCH, VD)
    residual = (block.astype(jnp.float32) + split_sum(mixed, v_out)).astype(jnp.bfloat16)
    normed_two = layer_norm(residual, vis_gain[1], vis_bias[1])
    inner = jax.nn.gelu(jnp.dot(normed_two, v_up, preferred_element_type=jnp.float32), approximate=False).astype(jnp.bfloat16)
    states = (residual.astype(jnp.float32) + split_sum(inner, v_down)).astype(jnp.bfloat16)
    return jnp.dot(pixel_shuffle(states), v_proj, preferred_element_type=jnp.float32).astype(jnp.bfloat16)

def decoder_layer(state, segment_ids, gain, w_query, w_kv, w_out):
    length = state.shape[0]
    positions = jnp.arange(length, dtype=jnp.int32)
    normed = rms_norm(state, gain)
    query = rotate(jnp.dot(normed, w_query, preferred_element_type=jnp.float32).reshape(length, QH, HD), positions).astype(jnp.bfloat16)
    keyed = rotate(jnp.dot(normed, w_kv[0], preferred_element_type=jnp.float32).reshape(length, KVH, HD), positions).astype(jnp.bfloat16)
    valued = jnp.dot(normed, w_kv[1], preferred_element_type=jnp.float32).astype(jnp.bfloat16).reshape(length, KVH, HD)
    grouped = query.reshape(length, KVH, QH // KVH, HD).astype(jnp.float32)
    scores = jnp.einsum('qkgd,skd->kgqs', grouped, keyed.astype(jnp.float32)) * HD ** (-0.5)
    allowed = (segment_ids[:, None] == segment_ids[None, :]) & (positions[None, :] <= positions[:, None])
    scores = jnp.where(allowed, scores, BLOCKED)
    probs = jax.nn.softmax(scores, axis=-1).astype(jnp.bfloat16)
    mixed = jnp.einsum('kgqs,skd->qkgd', probs.astype(jnp.float32), valued.astype(jnp.float32)).astype(jnp.bfloat16).reshape(length, QH * HD)
    return (state.astype(jnp.float32) + split_sum(mixed, w_out)).astype(jnp.bfloat16)

def reference(text, patches, segments, loss_mask, tile_batch, tile_offset, attn_gain, w_query, w_kv, w_out, vis_gain, vis_bias, v_qkv, v_out, v_up, v_down, v_proj):
    group_count = N_SECTION * N_DP
    grouped = patches.reshape(group_count, TILES_G * PATCH, VD)
    embedded = lax.map(lambda block: encode_group(block, vis_gain, vis_bias, v_qkv, v_out, v_up, v_down, v_proj), grouped)
    per_tile = embedded.reshape(N_SECTION, N_DP, TILES_G, POOL, D).transpose(1, 0, 2, 3, 4).reshape(N_DP, N_SECTION * TILES_G, POOL, D)
    states = text.reshape(MICRO, N_DP, L, D)
    places = tile_offset[:, :, None] + jnp.arange(POOL, dtype=jnp.int32)[None, None, :]
    dp_ids = jnp.broadcast_to(jnp.arange(N_DP, dtype=jnp.int32)[:, None, None], places.shape)
    micro_ids = jnp.broadcast_to(tile_batch[:, :, None], places.shape)
    states = states.at[micro_ids, dp_ids, places].set(per_tile)
    flat_states = states.reshape(MICRO * N_DP, L, D)
    flat_segments = segments.reshape(MICRO * N_DP, L)

    def run_sequence(pair):
        state, segment_ids = pair
        for layer_index in range(N_SECTION):
            state = decoder_layer(state, segment_ids, attn_gain[layer_index], w_query[layer_index], w_kv[layer_index], w_out[layer_index])
        return state
    hidden = lax.map(run_sequence, (flat_states, flat_segments)).reshape(MICRO, N_DP * L, D)
    weights = loss_mask.astype(jnp.float32)
    token_weight = weights * (MICRO * N_DP * L) / jnp.sum(weights)
    return (hidden, token_weight)
```

```python
import jax
import jax.numpy as jnp
from jax import lax
from jax.sharding import Mesh
from jax.sharding import PartitionSpec as P

HD = 128
VHD = 64
GRID = 16
PATCH = 256
POOL = 64
SECTION_DP = ("section", "dp_0", "dp_1")
SECTION_DP_MP = ("section", "dp_0", "dp_1", "mp")
DP = ("dp_0", "dp_1")
DP_MP = ("dp_0", "dp_1", "mp")


EPS = 1e-05
ROPE_BASE = 500000.0
BLOCKED = -1e30


def layer_norm(values, gain, bias):
    wide = values.astype(jnp.float32)
    center = wide - jnp.mean(wide, axis=-1, keepdims=True)
    spread = jnp.mean(center * center, axis=-1, keepdims=True)
    return (center * lax.rsqrt(spread + EPS) * gain + bias).astype(jnp.bfloat16)


def rms_norm(values, gain):
    wide = values.astype(jnp.float32)
    power = jnp.mean(wide * wide, axis=-1, keepdims=True)
    return (wide * lax.rsqrt(power + EPS) * gain).astype(jnp.bfloat16)


def pixel_shuffle(states):
    tile_count = states.shape[0] // PATCH
    side_half = GRID // 2
    width = states.shape[1]
    arranged = states.reshape(tile_count, side_half, 2, side_half, 2, width)
    return arranged.transpose(0, 1, 3, 2, 4, 5).reshape(
        tile_count * side_half * side_half, 4 * width
    )


def gathered(array, axis):
    copies = jnp.broadcast_to(array, (lax.axis_size(axis), *array.shape))
    return lax.all_to_all(copies, axis, split_axis=0, concat_axis=0, tiled=True)


def block_sum(partial_value):
    everything = gathered(partial_value.astype(jnp.bfloat16), "mp")
    return jnp.sum(everything.astype(jnp.float32), axis=0)


def transposed_dot(left, right):
    return lax.dot_general(
        left, right, (((1,), (1,)), ((), ())), preferred_element_type=jnp.float32
    )


def rope_tables(length):
    half_width = HD // 2
    freqs = ROPE_BASE ** (-2.0 * jnp.arange(half_width, dtype=jnp.float32) / HD)
    angles = jnp.arange(length, dtype=jnp.float32)[:, None] * freqs[None, :]
    cosine, sinus = jnp.cos(angles), jnp.sin(angles)
    return (
        jnp.concatenate([cosine, cosine], axis=1),
        jnp.concatenate([-sinus, sinus], axis=1),
    )


def encode_tiles(patches, vis_gain, vis_bias, small, proj_full):
    tile_count = patches.shape[0] // PATCH
    width = patches.shape[1]
    local = width // lax.axis_size("mp")
    head_count = local // VHD
    normed = layer_norm(patches, vis_gain[0], vis_bias[0])
    joined = jnp.dot(normed, small[:, : 3 * local], preferred_element_type=jnp.float32)
    joined = joined.astype(jnp.bfloat16).reshape(tile_count, PATCH, 3, head_count, VHD)
    query, keyed, valued = (joined[:, :, index] for index in range(3))
    scores = jnp.einsum("tqhd,tkhd->thqk", query, keyed, preferred_element_type=jnp.float32)
    probs = jax.nn.softmax(scores * VHD ** (-0.5), axis=-1).astype(jnp.bfloat16)
    mixed = jnp.einsum("thqk,tkhd->tqhd", probs, valued, preferred_element_type=jnp.float32)
    mixed = mixed.astype(jnp.bfloat16).reshape(tile_count * PATCH, local)
    attended = block_sum(transposed_dot(mixed, small[:, 3 * local : 4 * local]))
    residual = (patches.astype(jnp.float32) + attended).astype(jnp.bfloat16)
    normed_two = layer_norm(residual, vis_gain[1], vis_bias[1])
    hidden = small.shape[1] // 2 - 2 * local
    up = small[:, 4 * local : 4 * local + hidden]
    down = small[:, 4 * local + hidden :]
    inner = jax.nn.gelu(
        jnp.dot(normed_two, up, preferred_element_type=jnp.float32), approximate=False
    ).astype(jnp.bfloat16)
    fed = block_sum(transposed_dot(inner, down))
    states = (residual.astype(jnp.float32) + fed).astype(jnp.bfloat16)
    return jnp.dot(pixel_shuffle(states), proj_full, preferred_element_type=jnp.float32).astype(
        jnp.bfloat16
    )


def decoder_layer(state, allowed, cosine, sinus, w_joined, w_out):
    blocks = gathered(state, "mp")
    count, length, block_width = blocks.shape
    query_width = w_out.shape[0] // count
    rows = jnp.moveaxis(blocks, 0, 1).reshape(length, count * block_width)
    wide = rows.astype(jnp.float32)
    scale = lax.rsqrt(jnp.mean(wide * wide, axis=-1, keepdims=True) + EPS)
    joined = jnp.dot(rows, w_joined, preferred_element_type=jnp.float32) * scale
    heads = joined.reshape(length, joined.shape[1] // HD, HD)
    turned = heads * cosine[:, None] + jnp.roll(heads, HD // 2, axis=-1) * sinus[:, None]
    query_heads = query_width // HD
    query = turned[:, :query_heads].astype(jnp.bfloat16)
    keyed = turned[:, query_heads].astype(jnp.bfloat16)
    valued = heads[:, query_heads + 1].astype(jnp.bfloat16)
    scores = jnp.einsum("qgd,sd->gqs", query, keyed, preferred_element_type=jnp.float32)
    scores = jnp.where(allowed, scores * HD ** (-0.5), BLOCKED)
    probs = jax.nn.softmax(scores, axis=-1).astype(jnp.bfloat16)
    mixed = (
        jnp.einsum("gqs,sd->qgd", probs, valued, preferred_element_type=jnp.float32)
        .astype(jnp.bfloat16)
        .reshape(length, query_width)
    )
    parts = jnp.moveaxis(gathered(mixed, "mp"), 0, 1).reshape(length, count * query_width)
    added = jnp.dot(parts, w_out, preferred_element_type=jnp.float32)
    return (state.astype(jnp.float32) + added).astype(jnp.bfloat16)


def shards(
    text,
    patches,
    segments,
    loss_mask,
    tile_batch,
    tile_offset,
    attn_gain,
    w_query,
    w_kv,
    w_out,
    vis_gain,
    vis_bias,
    v_qkv,
    v_out,
    v_up,
    v_down,
    v_proj,
):
    sections = lax.axis_size("section")
    section_at = lax.axis_index("section")
    parts = lax.axis_size("mp")
    copies = lax.axis_size(DP)
    copy_at = lax.axis_index(DP)
    small = jnp.concatenate([v_qkv[0], v_qkv[1], v_qkv[2], v_out.T, v_up, v_down.T], axis=1)
    small = lax.all_gather(small, SECTION_DP, axis=0, tiled=True)
    proj_full = lax.all_gather(v_proj, SECTION_DP, axis=0, tiled=True)
    model_width = w_query.shape[1]
    row_share = model_width // copies
    pick = lambda array: lax.dynamic_slice_in_dim(array, copy_at * row_share, row_share, 0)
    own_rows = jnp.concatenate([pick(w_query[0]), pick(w_kv[0, 0]), pick(w_kv[0, 1])], axis=1)
    own_gain = lax.dynamic_slice_in_dim(attn_gain[0], copy_at * row_share, row_share, 0)
    own_rows = (own_rows.astype(jnp.float32) * own_gain[:, None]).astype(jnp.bfloat16)
    block_width = model_width // parts
    col_share = block_width // copies
    own_out = w_out[0].reshape(w_out.shape[1], parts, copies, col_share)
    own_out = lax.dynamic_slice_in_dim(own_out, copy_at, 1, 2)[:, :, 0]
    own_out = lax.all_to_all(
        jnp.moveaxis(own_out, 1, 0), "mp", split_axis=0, concat_axis=0, tiled=True
    )
    joined_all = lax.all_gather(own_rows, SECTION_DP).reshape(
        sections, model_width, own_rows.shape[1]
    )
    out_all = lax.all_gather(own_out, SECTION_DP).reshape(
        sections, copies, parts * w_out.shape[1], col_share
    )
    text_blocks = lax.all_to_all(
        jnp.moveaxis(text[0].reshape(text.shape[1], parts, block_width), 1, 0),
        "mp",
        split_axis=0,
        concat_axis=0,
        tiled=True,
    ).reshape(text.shape[1] * parts, block_width)
    embedded = encode_tiles(patches, vis_gain, vis_bias, small, proj_full)
    length = segments.shape[2]
    tiles_here = embedded.shape[0] // POOL
    batch_all = tile_batch[0]
    offset_all = tile_offset[0]
    own_batch = lax.dynamic_slice_in_dim(batch_all, section_at * tiles_here, tiles_here, 0)
    capacity = tiles_here // 2
    block_rows = capacity * POOL
    local_ids = jnp.arange(tiles_here, dtype=jnp.int32)
    local_same = (own_batch[:, None] == own_batch[None, :]) & (
        local_ids[None, :] < local_ids[:, None]
    )
    local_rank = jnp.sum(local_same.astype(jnp.int32), axis=1)
    send_rows = jnp.arange(sections * block_rows, dtype=jnp.int32)
    send_target = send_rows // block_rows
    send_rank = send_rows % block_rows // POOL
    send_match = (own_batch[None, :] == send_target[:, None]) & (
        local_rank[None, :] == send_rank[:, None]
    )
    own_rows = jnp.arange(tiles_here * POOL, dtype=jnp.int32)
    send_pick = jnp.repeat(send_match, POOL, axis=1) & (
        (own_rows % POOL)[None, :] == (send_rows % POOL)[:, None]
    )
    blocks = jnp.dot(
        send_pick.astype(jnp.bfloat16), embedded, preferred_element_type=jnp.float32
    ).astype(jnp.bfloat16)
    arrived = lax.all_to_all(blocks, "section", split_axis=0, concat_axis=0, tiled=True)
    tile_ids = jnp.arange(batch_all.shape[0], dtype=jnp.int32)
    source_ids = tile_ids // tiles_here
    tile_same = (
        (batch_all[:, None] == batch_all[None, :])
        & (source_ids[:, None] == source_ids[None, :])
        & (tile_ids[None, :] < tile_ids[:, None])
    )
    tile_rank = jnp.sum(tile_same.astype(jnp.int32), axis=1)
    slot_rows = jnp.arange(sections * block_rows, dtype=jnp.int32)
    slot_source = slot_rows // block_rows
    slot_rank = slot_rows % block_rows // POOL
    match = (
        (batch_all[None, :] == section_at)
        & (source_ids[None, :] == slot_source[:, None])
        & (tile_rank[None, :] == slot_rank[:, None])
    )
    slot_place = jnp.sum(match.astype(jnp.int32) * offset_all[None, :], axis=1) + slot_rows % POOL
    slot_valid = jnp.any(match, axis=1)
    places = jnp.arange(length, dtype=jnp.int32)
    picker = ((places[:, None] == slot_place[None, :]) & slot_valid[None, :]).astype(jnp.bfloat16)
    image_cols = jnp.dot(picker, arrived, preferred_element_type=jnp.float32).astype(jnp.bfloat16)
    covered = jnp.any(
        (batch_all[None, :] == section_at)
        & (places[:, None] >= offset_all[None, :])
        & (places[:, None] < offset_all[None, :] + POOL),
        axis=1,
    )
    state = jnp.where(covered[:, None], image_cols, text_blocks)
    segment_ids = segments[0, 0]
    allowed = (segment_ids[:, None] == segment_ids[None, :]) & (places[None, :] <= places[:, None])
    cosine, sinus = rope_tables(length)
    for layer in range(sections):
        w_layer = jnp.moveaxis(out_all[layer], 0, 1).reshape(out_all.shape[2], block_width)
        state = decoder_layer(state, allowed, cosine, sinus, joined_all[layer], w_layer)
    hidden = lax.all_to_all(
        state.reshape(parts, length // parts, block_width),
        "mp",
        split_axis=0,
        concat_axis=0,
        tiled=True,
    )
    hidden = jnp.moveaxis(hidden, 0, 1).reshape(length // parts, model_width)
    totals = lax.psum(jnp.sum(loss_mask), SECTION_DP_MP)
    scaling = float(sections * lax.axis_size(DP) * length)
    token_weight = loss_mask.astype(jnp.float32) * scaling / totals.astype(jnp.float32)
    return (hidden[None], token_weight)


def solution(mesh):
    split = Mesh(
        mesh.devices.reshape(mesh.shape["section"], 4, 2, mesh.shape["mp"]),
        ("section", "dp_0", "dp_1", "mp"),
    )
    return jax.shard_map(
        shards,
        mesh=split,
        in_specs=(
            P("section", DP_MP, None),
            P(SECTION_DP, None),
            P("section", DP, None),
            P("section", DP_MP),
            P(DP, None),
            P(DP, None),
            P("section", None),
            P("section", None, "mp"),
            P("section", None, None, "mp"),
            P("section", "mp", None),
            P(),
            P(),
            P(None, SECTION_DP, "mp"),
            P("mp", SECTION_DP),
            P(SECTION_DP, "mp"),
            P("mp", SECTION_DP),
            P(SECTION_DP, "mp"),
        ),
        out_specs=(P("section", DP_MP, None), P("section", DP_MP)),
        check_vma=False,
    )
```

```python
import jax
import jax.numpy as jnp
from jax import lax
from jax.experimental import pallas as pl
from jax.experimental.pallas import tpu as pltpu
from jax.sharding import Mesh
from jax.sharding import PartitionSpec as P

HD = 128
VHD = 64
GRID = 16
PATCH = 256
POOL = 64
SECTION_DP = ("section", "dp_0", "dp_1")
SECTION_DP_MP = ("section", "dp_0", "dp_1", "mp")
DP = ("dp_0", "dp_1")
DP_MP = ("dp_0", "dp_1", "mp")


EPS = 1e-05
ROPE_BASE = 500000.0
BLOCKED = -1e30
MESH = pl.DeviceIdType.MESH


def layer_norm(values, gain, bias):
    wide = values.astype(jnp.float32)
    center = wide - jnp.mean(wide, axis=-1, keepdims=True)
    spread = jnp.mean(center * center, axis=-1, keepdims=True)
    return (center * lax.rsqrt(spread + EPS) * gain + bias).astype(jnp.bfloat16)


def rms_norm(values, gain):
    wide = values.astype(jnp.float32)
    power = jnp.mean(wide * wide, axis=-1, keepdims=True)
    return (wide * lax.rsqrt(power + EPS) * gain).astype(jnp.bfloat16)


def pixel_shuffle(states):
    tile_count = states.shape[0] // PATCH
    side_half = GRID // 2
    width = states.shape[1]
    arranged = states.reshape(tile_count, side_half, 2, side_half, 2, width)
    return arranged.transpose(0, 1, 3, 2, 4, 5).reshape(
        tile_count * side_half * side_half, 4 * width
    )


def gathered(array, axis):
    copies = jnp.broadcast_to(array, (lax.axis_size(axis), *array.shape))
    return lax.all_to_all(copies, axis, split_axis=0, concat_axis=0, tiled=True)


def block_sum(partial_value):
    everything = gathered(partial_value.astype(jnp.bfloat16), "mp")
    return jnp.sum(everything.astype(jnp.float32), axis=0)


def transposed_dot(left, right):
    return lax.dot_general(
        left, right, (((1,), (1,)), ((), ())), preferred_element_type=jnp.float32
    )


def rope_tables(length):
    half_width = HD // 2
    freqs = ROPE_BASE ** (-2.0 * jnp.arange(half_width, dtype=jnp.float32) / HD)
    angles = jnp.arange(length, dtype=jnp.float32)[:, None] * freqs[None, :]
    cosine, sinus = jnp.cos(angles), jnp.sin(angles)
    return (
        jnp.concatenate([cosine, cosine], axis=1),
        jnp.concatenate([-sinus, sinus], axis=1),
    )


def encode_tiles(patches, vis_gain, vis_bias, small, proj_full):
    tile_count = patches.shape[0] // PATCH
    width = patches.shape[1]
    local = width // lax.axis_size("mp")
    head_count = local // VHD
    normed = layer_norm(patches, vis_gain[0], vis_bias[0])
    joined = jnp.dot(normed, small[:, : 3 * local], preferred_element_type=jnp.float32)
    joined = joined.astype(jnp.bfloat16).reshape(tile_count, PATCH, 3, head_count, VHD)
    query, keyed, valued = (joined[:, :, index] for index in range(3))
    scores = jnp.einsum("tqhd,tkhd->thqk", query, keyed, preferred_element_type=jnp.float32)
    probs = jax.nn.softmax(scores * VHD ** (-0.5), axis=-1).astype(jnp.bfloat16)
    mixed = jnp.einsum("thqk,tkhd->tqhd", probs, valued, preferred_element_type=jnp.float32)
    mixed = mixed.astype(jnp.bfloat16).reshape(tile_count * PATCH, local)
    attended = block_sum(transposed_dot(mixed, small[:, 3 * local : 4 * local]))
    residual = (patches.astype(jnp.float32) + attended).astype(jnp.bfloat16)
    normed_two = layer_norm(residual, vis_gain[1], vis_bias[1])
    hidden = small.shape[1] // 2 - 2 * local
    up = small[:, 4 * local : 4 * local + hidden]
    down = small[:, 4 * local + hidden :]
    inner = jax.nn.gelu(
        jnp.dot(normed_two, up, preferred_element_type=jnp.float32), approximate=False
    ).astype(jnp.bfloat16)
    fed = block_sum(transposed_dot(inner, down))
    states = (residual.astype(jnp.float32) + fed).astype(jnp.bfloat16)
    return jnp.dot(pixel_shuffle(states), proj_full, preferred_element_type=jnp.float32).astype(
        jnp.bfloat16
    )


def decoder_kernel(
    seg_col,
    seg_row,
    cos_ref,
    sin_ref,
    s0_ref,
    w_any,
    out_ref,
    xbuf,
    mbuf,
    wjb,
    wob,
    acc,
    ssq,
    kb,
    vb,
    bias,
    fin,
    hid,
    xs,
    xr,
    ms,
    mr,
    js,
    os,
    fs,
    fr,
):
    parts = 4
    layers = 4
    copies = w_any.shape[0] // layers
    length, block = s0_ref.shape
    half = length // 2
    joined = wjb.shape[2]
    query_width = wob.shape[1] // parts
    heads = query_width // HD
    depth = w_any.shape[1]
    col_share = wob.shape[2] // copies
    token_share = length // parts
    me = lax.axis_index("mp")
    right, opposite, left = (lax.rem(me + step, parts) for step in (1, 2, 3))

    def weight_copies(layer, par):
        found = []
        for d in range(copies):
            found.append(
                pltpu.make_async_copy(
                    w_any.at[layer * copies + d, :, pl.ds(0, joined)],
                    wjb.at[par, pl.ds(d * depth, depth), :],
                    js.at[par, d],
                )
            )
        for d in range(copies):
            for part in range(parts):
                found.append(
                    pltpu.make_async_copy(
                        w_any.at[
                            layer * copies + d, :, pl.ds(joined + part * col_share, col_share)
                        ],
                        wob.at[par, pl.ds(part * depth, depth), pl.ds(d * col_share, col_share)],
                        os.at[par, d * parts + part],
                    )
                )
        return found[:copies], found[copies:]

    def piece(buf, width, sends, recvs, par, h, kind, source, half_at, target):
        cols = pl.ds(pl.multiple_of(source * width + half_at * (width // 2), width // 2), width // 2)
        ref = buf.at[par, pl.ds(h * half, half), cols]
        return pltpu.make_async_remote_copy(
            src_ref=ref,
            dst_ref=ref,
            send_sem=sends.at[par, h, kind],
            recv_sem=recvs.at[par, h, kind],
            device_id={"mp": target},
            device_id_type=MESH,
        )

    def sent(kind, buf, width, sends, recvs, par, h):
        source, half_at, target = (
            (me, 0, right),
            (me, 1, right),
            (me, 1, left),
            (me, 0, left),
            (left, 0, right),
            (right, 1, left),
        )[kind]
        return piece(buf, width, sends, recvs, par, h, kind, source, half_at, target)

    def landed(kind, buf, width, sends, recvs, par, h):
        source, half_at = (
            (left, 0),
            (left, 1),
            (right, 1),
            (right, 0),
            (opposite, 0),
            (opposite, 1),
        )[kind]
        return piece(buf, width, sends, recvs, par, h, kind, source, half_at, right)

    x_args = (xbuf, block, xs, xr)
    m_args = (mbuf, query_width, ms, mr)

    def forward(args, par, h):
        landed(0, *args, par, h).wait_recv()
        sent(4, *args, par, h).start()
        landed(2, *args, par, h).wait_recv()
        sent(5, *args, par, h).start()

    def waits(args, par, h, kinds):
        for kind in kinds:
            landed(kind, *args, par, h).wait_recv()

    def wait_sends(args, par, h):
        for kind in range(6):
            sent(kind, *args, par, h).wait_send()

    def start_own(par, h):
        for kind in (0, 2, 1, 3):
            sent(kind, *x_args, par, h).start()

    first_joined, first_out = weight_copies(0, 0)
    for copy in first_joined + first_out:
        copy.start()
    barrier = pltpu.get_barrier_semaphore()
    for target in (right, opposite, left):
        pl.semaphore_signal(barrier, inc=1, device_id={"mp": target}, device_id_type=MESH)
    own_cols = pl.ds(pl.multiple_of(me * block, block), block)
    xbuf[0, :, own_cols] = s0_ref[...]
    pl.semaphore_wait(barrier, 3)
    for h in range(2):
        start_own(0, h)

    rows_at = lax.broadcasted_iota(jnp.int32, (length, length), 0)
    cols_at = lax.broadcasted_iota(jnp.int32, (length, length), 1)
    allowed = (seg_col[...] == seg_row[...]) & (cols_at <= rows_at)
    bias[...] = jnp.where(allowed, 0.0, BLOCKED)

    def project(par, h):
        rows = pl.ds(h * half, half)

        def add(source, first):
            cols = pl.ds(pl.multiple_of(source * block, block), block)
            values = xbuf[par, rows, cols]
            product = jnp.dot(values, wjb[par, cols, :], preferred_element_type=jnp.float32)
            wide = values.astype(jnp.float32)
            wide = wide * wide
            power = wide[:, :HD]
            for at in range(1, block // HD):
                power = power + wide[:, at * HD : (at + 1) * HD]
            if first:
                acc[:, :joined] = product
                ssq[...] = power
            else:
                acc[:, :joined] += product
                ssq[...] += power

        add(me, True)
        forward(x_args, par, h)
        waits(x_args, par, h, (1,))
        add(left, False)
        waits(x_args, par, h, (3,))
        add(right, False)
        waits(x_args, par, h, (4, 5))
        add(opposite, False)

    def attend(par, h):
        rows = pl.ds(h * half, half)
        keys = half * (h + 1)
        power = jnp.sum(ssq[...], axis=1, keepdims=True) * (1.0 / (parts * block))
        scale = lax.rsqrt(power + EPS)
        cosine = cos_ref[rows, :] * scale
        sinus = sin_ref[rows, :] * scale

        def turned(at):
            values = acc[:, at * HD : (at + 1) * HD]
            return values * cosine + pltpu.roll(values, HD // 2, 1) * sinus

        kb[rows, :] = turned(heads).astype(jnp.bfloat16)
        vb[rows, :] = (acc[:, (heads + 1) * HD : (heads + 2) * HD] * scale).astype(jnp.bfloat16)
        for head in range(heads):
            query = (turned(head) * HD ** (-0.5)).astype(jnp.bfloat16)
            scores = lax.dot_general(
                query,
                kb[:keys, :],
                (((1,), (1,)), ((), ())),
                preferred_element_type=jnp.float32,
            )
            scores = scores + bias[rows, :keys]
            top = jnp.max(scores, axis=1, keepdims=True)
            probs = jnp.exp(scores - top)
            total = jnp.sum(probs, axis=1, keepdims=True)
            mixed = jnp.dot(
                probs.astype(jnp.bfloat16), vb[:keys, :], preferred_element_type=jnp.float32
            )
            cols = pl.ds(pl.multiple_of(me * query_width + head * HD, HD), HD)
            mbuf[par, rows, cols] = (mixed / total).astype(jnp.bfloat16)
            if head == heads // 2 - 1:
                sent(0, *m_args, par, h).start()
                sent(3, *m_args, par, h).start()
                if h == 1:
                    forward(m_args, par, 0)
        sent(2, *m_args, par, h).start()
        sent(1, *m_args, par, h).start()

    def leave(par, h, layer):
        rows = pl.ds(h * half, half)
        if h == 1:
            forward(m_args, par, h)

        def term(source):
            cols = pl.ds(pl.multiple_of(source * query_width, query_width), query_width)
            return jnp.dot(
                mbuf[par, rows, cols], wob[par, cols, :], preferred_element_type=jnp.float32
            )

        acc[...] = xbuf[par, rows, own_cols].astype(jnp.float32) + term(me)
        waits(m_args, par, h, (1,))
        acc[...] += term(left)
        waits(m_args, par, h, (3,))
        acc[...] += term(right)
        waits(m_args, par, h, (4, 5))
        wait_sends(x_args, par, h)
        result = (acc[...] + term(opposite)).astype(jnp.bfloat16)

        @pl.when(layer < layers - 1)
        def _():
            xbuf[1 - par, rows, own_cols] = result
            start_own(1 - par, h)

        @pl.when(layer == layers - 1)
        def _():
            fin[rows, :] = result

    def one_layer(layer, carry):
        par = lax.rem(layer, 2)
        joined_copies, out_copies = weight_copies(layer, par)
        for copy in joined_copies:
            copy.wait()

        @pl.when(layer < layers - 1)
        def _():
            for copies_of in weight_copies(layer + 1, 1 - par):
                for copy in copies_of:
                    copy.start()

        for h in range(2):
            project(par, h)

            @pl.when(layer > 0)
            def _():
                wait_sends(m_args, 1 - par, h)

            attend(par, h)
        for copy in out_copies:
            copy.wait()
        for h in range(2):
            leave(par, h, layer)
        return carry

    lax.fori_loop(0, layers, one_layer, 0)
    last = (layers - 1) % 2

    def shared(step):
        target = lax.rem(me + step, parts)
        return pltpu.make_async_remote_copy(
            src_ref=fin.at[pl.ds(pl.multiple_of(target * token_share, token_share), token_share), :],
            dst_ref=hid.at[:, own_cols],
            send_sem=fs.at[step - 1],
            recv_sem=fr.at[step - 1],
            device_id={"mp": target},
            device_id_type=MESH,
        )

    for step in (2, 1, 3):
        shared(step).start()
    hid[:, own_cols] = fin[pl.ds(pl.multiple_of(me * token_share, token_share), token_share), :]
    for h in range(2):
        wait_sends(m_args, last, h)
    for step in (2, 1, 3):
        shared(step).wait()
    out_ref[...] = hid[...]


def decode(state, segment_ids, weights):
    length, block = state.shape
    parts = lax.axis_size("mp")
    copies = lax.axis_size(DP)
    depth = weights.shape[1]
    joined = weights.shape[2] - parts * (block // copies)
    cosine, sinus = rope_tables(length)
    dma = pltpu.SemaphoreType.DMA
    vmem = pl.BlockSpec(memory_space=pltpu.VMEM)
    return pl.pallas_call(
        decoder_kernel,
        out_shape=jax.ShapeDtypeStruct((length // parts, parts * block), jnp.bfloat16),
        in_specs=[vmem] * 5 + [pl.BlockSpec(memory_space=pl.ANY)],
        out_specs=vmem,
        scratch_shapes=[
            pltpu.VMEM((2, length, parts * block), jnp.bfloat16),
            pltpu.VMEM((2, length, parts * depth), jnp.bfloat16),
            pltpu.VMEM((2, copies * depth, joined), jnp.bfloat16),
            pltpu.VMEM((2, parts * depth, block), jnp.bfloat16),
            pltpu.VMEM((length // 2, block), jnp.float32),
            pltpu.VMEM((length // 2, HD), jnp.float32),
            pltpu.VMEM((length, HD), jnp.bfloat16),
            pltpu.VMEM((length, HD), jnp.bfloat16),
            pltpu.VMEM((length, length), jnp.float32),
            pltpu.VMEM((length, block), jnp.bfloat16),
            pltpu.VMEM((length // parts, parts * block), jnp.bfloat16),
            dma((2, 2, 6)),
            dma((2, 2, 6)),
            dma((2, 2, 6)),
            dma((2, 2, 6)),
            dma((2, copies)),
            dma((2, copies * parts)),
            dma((3,)),
            dma((3,)),
        ],
        compiler_params=pltpu.CompilerParams(
            collective_id=0, has_side_effects=True, vmem_limit_bytes=60 * 1024 * 1024
        ),
    )(segment_ids[:, None], segment_ids[None, :], cosine, sinus, state, weights)


def shards(
    text,
    patches,
    segments,
    loss_mask,
    tile_batch,
    tile_offset,
    attn_gain,
    w_query,
    w_kv,
    w_out,
    vis_gain,
    vis_bias,
    v_qkv,
    v_out,
    v_up,
    v_down,
    v_proj,
):
    sections = lax.axis_size("section")
    section_at = lax.axis_index("section")
    parts = lax.axis_size("mp")
    copies = lax.axis_size(DP)
    copy_at = lax.axis_index(DP)
    totals = jnp.sum(loss_mask)
    for axis in SECTION_DP_MP:
        totals = lax.psum(totals, axis)
    small = jnp.concatenate([v_qkv[0], v_qkv[1], v_qkv[2], v_out.T, v_up, v_down.T], axis=1)
    small = lax.all_gather(small, SECTION_DP, axis=0, tiled=True)
    proj_full = lax.all_gather(v_proj, SECTION_DP, axis=0, tiled=True)
    model_width = w_query.shape[1]
    row_share = model_width // copies
    pick = lambda array: lax.dynamic_slice_in_dim(array, copy_at * row_share, row_share, 0)
    own_rows = jnp.concatenate([pick(w_query[0]), pick(w_kv[0, 0]), pick(w_kv[0, 1])], axis=1)
    own_gain = lax.dynamic_slice_in_dim(attn_gain[0], copy_at * row_share, row_share, 0)
    own_rows = (own_rows.astype(jnp.float32) * own_gain[:, None]).astype(jnp.bfloat16)
    block_width = model_width // parts
    col_share = block_width // copies
    own_out = w_out[0].reshape(w_out.shape[1], parts, copies, col_share)
    own_out = lax.dynamic_slice_in_dim(own_out, copy_at, 1, 2)[:, :, 0]
    own_out = lax.all_to_all(
        jnp.moveaxis(own_out, 1, 0), "mp", split_axis=0, concat_axis=0, tiled=True
    )
    own_out, totals = lax.optimization_barrier((own_out, totals))
    own_out = jnp.moveaxis(own_out, 0, 1).reshape(w_out.shape[1], parts * col_share)
    weights = lax.all_gather(jnp.concatenate([own_rows, own_out], axis=1), SECTION_DP)
    text_blocks = lax.all_to_all(
        jnp.moveaxis(text[0].reshape(text.shape[1], parts, block_width), 1, 0),
        "mp",
        split_axis=0,
        concat_axis=0,
        tiled=True,
    ).reshape(text.shape[1] * parts, block_width)
    patches, totals, text_blocks = lax.optimization_barrier((patches, totals, text_blocks))
    embedded = encode_tiles(patches, vis_gain, vis_bias, small, proj_full)
    length = segments.shape[2]
    tiles_here = embedded.shape[0] // POOL
    batch_all = tile_batch[0]
    offset_all = tile_offset[0]
    own_batch = lax.dynamic_slice_in_dim(batch_all, section_at * tiles_here, tiles_here, 0)
    capacity = tiles_here // 2
    block_rows = capacity * POOL
    local_ids = jnp.arange(tiles_here, dtype=jnp.int32)
    local_same = (own_batch[:, None] == own_batch[None, :]) & (
        local_ids[None, :] < local_ids[:, None]
    )
    local_rank = jnp.sum(local_same.astype(jnp.int32), axis=1)
    send_rows = jnp.arange(sections * block_rows, dtype=jnp.int32)
    send_target = send_rows // block_rows
    send_rank = send_rows % block_rows // POOL
    send_match = (own_batch[None, :] == send_target[:, None]) & (
        local_rank[None, :] == send_rank[:, None]
    )
    own_rows = jnp.arange(tiles_here * POOL, dtype=jnp.int32)
    send_pick = jnp.repeat(send_match, POOL, axis=1) & (
        (own_rows % POOL)[None, :] == (send_rows % POOL)[:, None]
    )
    blocks = jnp.dot(
        send_pick.astype(jnp.bfloat16), embedded, preferred_element_type=jnp.float32
    ).astype(jnp.bfloat16)
    arrived = lax.all_to_all(blocks, "section", split_axis=0, concat_axis=0, tiled=True)
    tile_ids = jnp.arange(batch_all.shape[0], dtype=jnp.int32)
    source_ids = tile_ids // tiles_here
    tile_same = (
        (batch_all[:, None] == batch_all[None, :])
        & (source_ids[:, None] == source_ids[None, :])
        & (tile_ids[None, :] < tile_ids[:, None])
    )
    tile_rank = jnp.sum(tile_same.astype(jnp.int32), axis=1)
    slot_rows = jnp.arange(sections * block_rows, dtype=jnp.int32)
    slot_source = slot_rows // block_rows
    slot_rank = slot_rows % block_rows // POOL
    match = (
        (batch_all[None, :] == section_at)
        & (source_ids[None, :] == slot_source[:, None])
        & (tile_rank[None, :] == slot_rank[:, None])
    )
    slot_place = jnp.sum(match.astype(jnp.int32) * offset_all[None, :], axis=1) + slot_rows % POOL
    slot_valid = jnp.any(match, axis=1)
    places = jnp.arange(length, dtype=jnp.int32)
    picker = ((places[:, None] == slot_place[None, :]) & slot_valid[None, :]).astype(jnp.bfloat16)
    image_cols = jnp.dot(picker, arrived, preferred_element_type=jnp.float32).astype(jnp.bfloat16)
    covered = jnp.any(
        (batch_all[None, :] == section_at)
        & (places[:, None] >= offset_all[None, :])
        & (places[:, None] < offset_all[None, :] + POOL),
        axis=1,
    )
    state = jnp.where(covered[:, None], image_cols, text_blocks)
    segment_ids = segments[0, 0]
    hidden = decode(state, segment_ids, weights)
    scaling = float(sections * lax.axis_size(DP) * length)
    token_weight = loss_mask.astype(jnp.float32) * scaling / totals.astype(jnp.float32)
    return (hidden[None], token_weight)


def solution(mesh):
    split = Mesh(
        mesh.devices.reshape(mesh.shape["section"], 4, 2, mesh.shape["mp"]),
        ("section", "dp_0", "dp_1", "mp"),
    )
    return jax.shard_map(
        shards,
        mesh=split,
        in_specs=(
            P("section", DP_MP, None),
            P(SECTION_DP, None),
            P("section", DP, None),
            P("section", DP_MP),
            P(DP, None),
            P(DP, None),
            P("section", None),
            P("section", None, "mp"),
            P("section", None, None, "mp"),
            P("section", "mp", None),
            P(),
            P(),
            P(None, SECTION_DP, "mp"),
            P("mp", SECTION_DP),
            P(SECTION_DP, "mp"),
            P("mp", SECTION_DP),
            P(SECTION_DP, "mp"),
        ),
        out_specs=(P("section", DP_MP, None), P("section", DP_MP)),
        check_vma=False,
    )
```

```python
import jax
import jax.numpy as jnp
from jax import lax
from jax.experimental import pallas as pl
from jax.experimental.pallas import tpu as pltpu
from jax.sharding import Mesh
from jax.sharding import PartitionSpec as P

HD = 128
VHD = 64
GRID = 16
PATCH = 256
POOL = 64
SECTION_DP = ("section", "dp_0", "dp_1")
SECTION_DP_MP = ("section", "dp_0", "dp_1", "mp")
DP = ("dp_0", "dp_1")
DP_MP = ("dp_0", "dp_1", "mp")


EPS = 1e-05
ROPE_BASE = 500000.0
BLOCKED = -1e30
MESH = pl.DeviceIdType.MESH


def rope_tables(length):
    half_width = HD // 2
    freqs = ROPE_BASE ** (-2.0 * jnp.arange(half_width, dtype=jnp.float32) / HD)
    angles = jnp.arange(length, dtype=jnp.float32)[:, None] * freqs[None, :]
    cosine, sinus = jnp.cos(angles), jnp.sin(angles)
    return (
        jnp.concatenate([cosine, cosine], axis=1),
        jnp.concatenate([-sinus, sinus], axis=1),
    )


def vision_kernel(
    patches_ref,
    gain_ref,
    bias_ref,
    text_ref,
    mask_ref,
    own_ref,
    place_ref,
    small_ref,
    proj_ref,
    state_ref,
    weight_ref,
    sm,
    pj,
    joined,
    mix,
    part,
    rsb,
    res,
    n2,
    pooled,
    blk,
    arrived,
    txt,
    cbuf,
    gs,
    gr,
    xs,
    xr,
    zs,
    zr,
    ts,
    tr,
    cs,
    cr,
    loc,
):
    parts = 4
    z, y, c, me = (lax.axis_index(name) for name in ("section", "dp_0", "dp_1", "mp"))
    rows, width = patches_ref.shape
    tiles = rows // PATCH
    share = PATCH // parts
    local = width // parts
    hidden = small_ref.shape[1] // 2 - 2 * local
    block = text_ref.shape[1] // parts
    token_share = text_ref.shape[0]
    pool_share = POOL // parts

    def place_of(core, first, second):
        return first * (8 - 6 * core) + second * (2 + 6 * core) + core

    a, b = z * (1 - c) + y * c, y * (1 - c) + z * c
    pa, pb = z * c + y * (1 - c), y * c + z * (1 - c)

    def along_a(step):
        return {"section": lax.rem(z + (1 - c) * step, 4), "dp_0": lax.rem(y + c * step, 4)}

    def along_b(step):
        return {"section": lax.rem(z + c * step, 4), "dp_0": lax.rem(y + (1 - c) * step, 4)}

    def along_x(step):
        return {"mp": lax.rem(me + step, parts)}

    partner = {"dp_1": 1 - c}
    full, own_piece = (sm, pj), (small_ref, proj_ref)

    def remote(src, dst, send, recv, target):
        return pltpu.make_async_remote_copy(
            src_ref=src,
            dst_ref=dst,
            send_sem=send,
            recv_sem=recv,
            device_id=target,
            device_id_type=MESH,
        )

    def region(arr, core, first, second):
        count = own_piece[arr].shape[0]
        at = place_of(core, lax.rem(first, 4), lax.rem(second, 4))
        return full[arr].at[pl.ds(pl.multiple_of(at * count, count), count), :]

    def share_out(arr, kind, ra, rb, target):
        dst = region(arr, c, a + ra, b + rb)
        src = own_piece[arr] if (ra, rb) == (0, 0) else dst
        return remote(src, dst, gs.at[arr, kind], gr.at[arr, kind], target)

    started = ([], [])

    def give(arr, kind, ra, rb, target):
        copy = share_out(arr, kind, ra, rb, target)
        copy.start()
        started[arr].append(copy)

    def take(arr, kind, ra, rb):
        share_out(arr, kind, ra, rb, partner).wait_recv()

    def to_both(arr, ra):
        give(arr, 3 + ra, ra, 0, along_b(1))
        give(arr, 7 + ra, ra, 0, along_b(3))
        give(arr, 15 + ra * 4, ra, 0, partner)

    def gather_start(arr):
        give(arr, 0, 0, 0, along_a(1))
        give(arr, 1, 0, 0, along_a(3))
        to_both(arr, 0)
        pltpu.make_async_copy(own_piece[arr], region(arr, c, a, b), loc.at[arr]).start()

    def gather_a(arr):
        take(arr, 0, 3, 0)
        if arr == 0:
            give(arr, 2, 3, 0, along_a(1))
        to_both(arr, 3)
        take(arr, 1, 1, 0)
        if arr == 1:
            give(arr, 2, 1, 0, along_a(3))
        to_both(arr, 1)
        take(arr, 2, 2, 0)
        to_both(arr, 2)

    def gather_b(arr):
        for ra in (0, 3, 1, 2):
            take(arr, 3 + ra, ra, 3)
            if ra < 2:
                give(arr, 11 + ra, ra, 3, along_b(1))
            give(arr, 15 + ra * 4 + 3, ra, 3, partner)
            take(arr, 7 + ra, ra, 1)
            if ra >= 2:
                give(arr, 11 + ra, ra, 1, along_b(3))
            give(arr, 15 + ra * 4 + 1, ra, 1, partner)

    def gather_b2(arr):
        for ra in (0, 3, 1, 2):
            take(arr, 11 + ra, ra, 2)
            give(arr, 15 + ra * 4 + 2, ra, 2, partner)

    def gather_end(arr):
        for ra in range(4):
            for rb in range(4):
                kind = 15 + ra * 4 + rb
                dst = region(arr, 1 - c, pa + ra, pb + rb)
                remote(dst, dst, gs.at[arr, kind], gr.at[arr, kind], partner).wait_recv()
        pltpu.make_async_copy(own_piece[arr], region(arr, c, a, b), loc.at[arr]).wait()

    def count_copy(stage, step):
        name = ("mp", "dp_1", "dp_0", "section")[stage]
        at = (me, c, y, z)[stage]
        size = (4, 2, 4, 4)[stage]
        return remote(
            cbuf.at[stage, 3],
            cbuf.at[stage, step - 1],
            cs.at[stage, step - 1],
            cr.at[stage, step - 1],
            {name: lax.rem(at + step, size)},
        )

    def count_steps(stage):
        return (1,) if stage == 1 else (1, 2, 3)

    def count_send(stage):
        for step in count_steps(stage):
            count_copy(stage, step).start()

    def count_sum(stage):
        total = cbuf[stage, 3]
        for step in count_steps(stage):
            count_copy(stage, step).wait()
            total = total + cbuf[stage, step - 1]
        return total

    def text_copy(step):
        target = lax.rem(me + step, parts)
        return remote(
            text_ref.at[:, pl.ds(pl.multiple_of(target * block, block), block)],
            txt.at[pl.ds(pl.multiple_of(me * token_share, token_share), token_share), :],
            ts.at[step - 1],
            tr.at[step - 1],
            along_x(step),
        )

    def scatter_copy(stage, tile, step):
        target = lax.rem(me + step, parts)
        return remote(
            part.at[stage, tile, pl.ds(pl.multiple_of(target * share, share), share), :],
            rsb.at[stage, tile, step - 1],
            xs.at[2 * stage, tile, step - 1],
            xr.at[2 * stage, tile, step - 1],
            along_x(step),
        )

    def spread_copy(stage, tile, step):
        if stage == 0:
            ref = n2.at[tile, pl.ds(pl.multiple_of(me * share, share), share), :]
        else:
            ref = pooled.at[
                pl.ds(pl.multiple_of(tile * POOL + me * pool_share, pool_share), pool_share), :
            ]
        return remote(
            ref, ref, xs.at[2 * stage + 1, tile, step - 1], xr.at[2 * stage + 1, tile, step - 1], along_x(step)
        )

    def normed(wide, at):
        center = wide - jnp.mean(wide, axis=1, keepdims=True)
        spread = jnp.mean(center * center, axis=1, keepdims=True)
        scaled = center * lax.rsqrt(spread + EPS) * gain_ref[at : at + 1, :]
        return (scaled + bias_ref[at : at + 1, :]).astype(jnp.bfloat16)

    def own_sum(stage, tile):
        mine = pl.ds(pl.multiple_of(me * share, share), share)
        total = part[stage, tile, mine, :].astype(jnp.float32)
        for step in (1, 3, 2):
            scatter_copy(stage, tile, step).wait()
            total = total + rsb[stage, tile, step - 1].astype(jnp.float32)
        return total

    barrier = pltpu.get_barrier_semaphore()
    others = [{"section": lax.rem(z + step, 4)} for step in (1, 2, 3)]
    others += [{"dp_0": lax.rem(y + step, 4)} for step in (1, 2, 3)]
    others += [along_x(step) for step in (1, 2, 3)] + [partner]
    for target in others:
        pl.semaphore_signal(barrier, inc=1, device_id=target, device_id_type=MESH)
    mask = mask_ref[...].astype(jnp.float32)
    cbuf[0, 3] = jnp.broadcast_to(jnp.sum(mask, axis=1, keepdims=True), cbuf.shape[2:])
    pl.semaphore_wait(barrier, len(others))
    gather_start(0)
    gather_start(1)
    for step in (1, 3, 2):
        text_copy(step).start()
    count_send(0)
    own_rows = pl.ds(pl.multiple_of(me * token_share, token_share), token_share)
    txt[own_rows, :] = text_ref[:, pl.ds(pl.multiple_of(me * block, block), block)]
    first = normed(patches_ref[...].astype(jnp.float32), 0)
    gather_a(0)
    gather_a(1)
    gather_b(0)
    gather_b2(0)
    cbuf[1, 3] = count_sum(0)
    count_send(1)
    gather_end(0)
    joined[...] = jnp.dot(first, sm[:, : 3 * local], preferred_element_type=jnp.float32)
    low = lax.broadcasted_iota(jnp.int32, (PATCH, 2 * VHD), 1) < VHD

    def attend(tile):
        at = pl.ds(tile * PATCH, PATCH)
        for pair in range(local // (2 * VHD)):
            start = pair * 2 * VHD
            query = joined[at, start : start + 2 * VHD]
            keyed = joined[at, local + start : local + start + 2 * VHD].astype(jnp.bfloat16)
            valued = joined[at, 2 * local + start : 2 * local + start + 2 * VHD]
            valued = valued.astype(jnp.bfloat16)
            found = []
            for side in (low, jnp.logical_not(low)):
                masked = jnp.where(side, query, 0.0).astype(jnp.bfloat16)
                scores = lax.dot_general(
                    masked, keyed, (((1,), (1,)), ((), ())), preferred_element_type=jnp.float32
                )
                scores = scores * VHD ** (-0.5)
                probs = jnp.exp(scores - jnp.max(scores, axis=1, keepdims=True))
                total = jnp.sum(probs, axis=1, keepdims=True)
                product = jnp.dot(
                    probs.astype(jnp.bfloat16), valued, preferred_element_type=jnp.float32
                )
                found.append(product / total)
            mix[at, start : start + 2 * VHD] = jnp.where(low, *found).astype(jnp.bfloat16)
        partial_sum = lax.dot_general(
            mix[at, :],
            sm[:, 3 * local : 4 * local],
            (((1,), (1,)), ((), ())),
            preferred_element_type=jnp.float32,
        )
        part[0, tile] = partial_sum.astype(jnp.bfloat16)
        for step in (1, 3, 2):
            scatter_copy(0, tile, step).start()

    def middle(tile):
        mine = pl.ds(pl.multiple_of(tile * PATCH + me * share, share), share)
        total = patches_ref[mine, :].astype(jnp.float32) + own_sum(0, tile)
        kept = total.astype(jnp.bfloat16)
        res[tile] = kept
        rows_here = pl.ds(pl.multiple_of(me * share, share), share)
        n2[tile, rows_here, :] = normed(kept.astype(jnp.float32), 1)
        for step in (1, 3, 2):
            spread_copy(0, tile, step).start()

    def expand(tile):
        for step in (1, 3, 2):
            spread_copy(0, tile, step).wait()
        inner = jnp.dot(
            n2[tile],
            sm[:, 4 * local : 4 * local + hidden],
            preferred_element_type=jnp.float32,
        )
        inner = (0.5 * inner * (1.0 + lax.erf(inner * 0.5**0.5))).astype(jnp.bfloat16)
        partial_sum = lax.dot_general(
            inner,
            sm[:, 4 * local + hidden :],
            (((1,), (1,)), ((), ())),
            preferred_element_type=jnp.float32,
        )
        part[1, tile] = partial_sum.astype(jnp.bfloat16)
        for step in (1, 3, 2):
            scatter_copy(1, tile, step).start()

    row_at = lax.broadcasted_iota(jnp.int32, (share, share), 0)
    col_at = lax.broadcasted_iota(jnp.int32, (share, share), 1)
    quad, token = row_at // pool_share, row_at % pool_share
    side = GRID // 2
    origin = 2 * GRID * (token // side) + GRID * (quad // 2) + 2 * (token % side) + quad % 2
    shuffle = (col_at == origin).astype(jnp.float32).astype(jnp.bfloat16)

    def pool(tile):
        kept = (res[tile].astype(jnp.float32) + own_sum(1, tile)).astype(jnp.bfloat16)
        moved = jnp.dot(shuffle, kept, preferred_element_type=jnp.float32).astype(jnp.bfloat16)
        mine = pl.ds(pl.multiple_of(tile * POOL + me * pool_share, pool_share), pool_share)
        for at in range(4):
            pooled[mine, at * width : (at + 1) * width] = moved[
                at * pool_share : (at + 1) * pool_share, :
            ]
        for step in (1, 3, 2):
            spread_copy(1, tile, step).start()

    attend(0)
    gather_b(1)
    attend(1)
    middle(0)
    gather_b2(1)
    middle(1)
    cbuf[2, 3] = count_sum(1)
    count_send(2)
    for tile in range(tiles):
        expand(tile)
    for tile in range(tiles):
        pool(tile)
    cbuf[3, 3] = count_sum(2)
    count_send(3)
    gather_end(1)
    for tile in range(tiles):
        for step in (1, 3, 2):
            spread_copy(1, tile, step).wait()
    image = jnp.dot(pooled[...], pj[...], preferred_element_type=jnp.float32).astype(jnp.bfloat16)
    send_row = lax.broadcasted_iota(jnp.int32, (4 * POOL, tiles * POOL), 0)
    send_col = lax.broadcasted_iota(jnp.int32, (4 * POOL, tiles * POOL), 1)
    chosen = (own_ref[...] == send_row // POOL) & (send_row % POOL == send_col % POOL)
    chosen = chosen.astype(jnp.float32).astype(jnp.bfloat16)
    blk[...] = jnp.dot(chosen, image, preferred_element_type=jnp.float32).astype(jnp.bfloat16)

    def home_copy(step):
        target = lax.rem(z + step, 4)
        return remote(
            blk.at[pl.ds(pl.multiple_of(target * POOL, POOL), POOL), :],
            arrived.at[pl.ds(pl.multiple_of(z * POOL, POOL), POOL), :],
            zs.at[step - 1],
            zr.at[step - 1],
            {"section": target},
        )

    for step in (2, 1, 3):
        home_copy(step).start()
    here = pl.ds(pl.multiple_of(z * POOL, POOL), POOL)
    arrived[here, :] = blk[here, :]
    count = count_sum(3)
    scaling = float(4 * 8 * parts * token_share)
    weight_ref[...] = mask * scaling / count[:1, :]
    length = state_ref.shape[0]
    picked = lax.broadcasted_iota(jnp.int32, (length, 4 * POOL), 0) == place_ref[...]
    picked = picked.astype(jnp.float32)
    covered = jnp.max(picked, axis=1, keepdims=True) > 0.5
    for step in (1, 3, 2):
        text_copy(step).wait()
    for copies_of in started:
        for copy in copies_of:
            copy.wait_send()
    for step in (1, 3, 2):
        home_copy(step).wait()
    placed = jnp.dot(
        picked.astype(jnp.bfloat16), arrived[...], preferred_element_type=jnp.float32
    )
    state_ref[...] = jnp.where(covered, placed, txt[...].astype(jnp.float32)).astype(jnp.bfloat16)


def encode(patches, vis_gain, vis_bias, text, mask, own, place, small, proj):
    rows, width = patches.shape
    tiles = rows // PATCH
    block = text.shape[1] // 4
    length = text.shape[0] * 4
    share = PATCH // 4
    dma = pltpu.SemaphoreType.DMA
    vmem = pl.BlockSpec(memory_space=pltpu.VMEM)
    bf16 = jnp.bfloat16
    return pl.pallas_call(
        vision_kernel,
        out_shape=(
            jax.ShapeDtypeStruct((length, block), bf16),
            jax.ShapeDtypeStruct(mask.shape, jnp.float32),
        ),
        in_specs=[vmem] * 9,
        out_specs=(vmem, vmem),
        scratch_shapes=[
            pltpu.VMEM((small.shape[0] * 32, small.shape[1]), bf16),
            pltpu.VMEM((proj.shape[0] * 32, proj.shape[1]), bf16),
            pltpu.VMEM((rows, 3 * width // 4), jnp.float32),
            pltpu.VMEM((rows, width // 4), bf16),
            pltpu.VMEM((2, tiles, PATCH, width), bf16),
            pltpu.VMEM((2, tiles, 3, share, width), bf16),
            pltpu.VMEM((tiles, share, width), bf16),
            pltpu.VMEM((tiles, PATCH, width), bf16),
            pltpu.VMEM((tiles * POOL, 4 * width), bf16),
            pltpu.VMEM((4 * POOL, block), bf16),
            pltpu.VMEM((4 * POOL, block), bf16),
            pltpu.VMEM((length, block), bf16),
            pltpu.VMEM((4, 4, 8, 128), jnp.float32),
            dma((2, 31)),
            dma((2, 31)),
            dma((4, tiles, 3)),
            dma((4, tiles, 3)),
            dma((3,)),
            dma((3,)),
            dma((3,)),
            dma((3,)),
            dma((4, 3)),
            dma((4, 3)),
            dma((2,)),
        ],
        compiler_params=pltpu.CompilerParams(
            collective_id=1, has_side_effects=True, vmem_limit_bytes=56 * 1024 * 1024
        ),
    )(patches, vis_gain, vis_bias, text, mask, own, place, small, proj)


def decoder_kernel(
    seg_col,
    seg_row,
    cos_ref,
    sin_ref,
    s0_ref,
    w_any,
    out_ref,
    xbuf,
    mbuf,
    wjb,
    wob,
    acc,
    ssq,
    kb,
    vb,
    bias,
    fin,
    hid,
    xs,
    xr,
    ms,
    mr,
    js,
    os,
    fs,
    fr,
):
    parts = 4
    layers = 4
    copies = w_any.shape[0] // layers
    length, block = s0_ref.shape
    half = length // 2
    joined = wjb.shape[2]
    query_width = wob.shape[1] // parts
    heads = query_width // HD
    depth = w_any.shape[1]
    col_share = wob.shape[2] // copies
    token_share = length // parts
    me = lax.axis_index("mp")
    right, opposite, left = (lax.rem(me + step, parts) for step in (1, 2, 3))

    def weight_copies(layer, par):
        found = []
        for d in range(copies):
            found.append(
                pltpu.make_async_copy(
                    w_any.at[layer * copies + d, :, pl.ds(0, joined)],
                    wjb.at[par, pl.ds(d * depth, depth), :],
                    js.at[par, d],
                )
            )
        for d in range(copies):
            for part in range(parts):
                found.append(
                    pltpu.make_async_copy(
                        w_any.at[
                            layer * copies + d, :, pl.ds(joined + part * col_share, col_share)
                        ],
                        wob.at[par, pl.ds(part * depth, depth), pl.ds(d * col_share, col_share)],
                        os.at[par, d * parts + part],
                    )
                )
        return found[:copies], found[copies:]

    def piece(buf, width, sends, recvs, par, h, kind, source, half_at, target):
        cols = pl.ds(pl.multiple_of(source * width + half_at * (width // 2), width // 2), width // 2)
        ref = buf.at[par, pl.ds(h * half, half), cols]
        return pltpu.make_async_remote_copy(
            src_ref=ref,
            dst_ref=ref,
            send_sem=sends.at[par, h, kind],
            recv_sem=recvs.at[par, h, kind],
            device_id={"mp": target},
            device_id_type=MESH,
        )

    def sent(kind, buf, width, sends, recvs, par, h):
        source, half_at, target = (
            (me, 0, right),
            (me, 1, right),
            (me, 1, left),
            (me, 0, left),
            (left, 0, right),
            (right, 1, left),
        )[kind]
        return piece(buf, width, sends, recvs, par, h, kind, source, half_at, target)

    def landed(kind, buf, width, sends, recvs, par, h):
        source, half_at = (
            (left, 0),
            (left, 1),
            (right, 1),
            (right, 0),
            (opposite, 0),
            (opposite, 1),
        )[kind]
        return piece(buf, width, sends, recvs, par, h, kind, source, half_at, right)

    x_args = (xbuf, block, xs, xr)
    m_args = (mbuf, query_width, ms, mr)

    def forward(args, par, h):
        landed(0, *args, par, h).wait_recv()
        sent(4, *args, par, h).start()
        landed(2, *args, par, h).wait_recv()
        sent(5, *args, par, h).start()

    def waits(args, par, h, kinds):
        for kind in kinds:
            landed(kind, *args, par, h).wait_recv()

    def wait_sends(args, par, h):
        for kind in range(6):
            sent(kind, *args, par, h).wait_send()

    def start_own(par, h):
        for kind in (0, 2, 1, 3):
            sent(kind, *x_args, par, h).start()

    first_joined, first_out = weight_copies(0, 0)
    for copy in first_joined + first_out:
        copy.start()
    barrier = pltpu.get_barrier_semaphore()
    for target in (right, opposite, left):
        pl.semaphore_signal(barrier, inc=1, device_id={"mp": target}, device_id_type=MESH)
    own_cols = pl.ds(pl.multiple_of(me * block, block), block)
    xbuf[0, :, own_cols] = s0_ref[...]
    pl.semaphore_wait(barrier, 3)
    for h in range(2):
        start_own(0, h)

    rows_at = lax.broadcasted_iota(jnp.int32, (length, length), 0)
    cols_at = lax.broadcasted_iota(jnp.int32, (length, length), 1)
    allowed = (seg_col[...] == seg_row[...]) & (cols_at <= rows_at)
    bias[...] = jnp.where(allowed, 0.0, BLOCKED)

    def project(par, h):
        rows = pl.ds(h * half, half)

        def add(source, first):
            cols = pl.ds(pl.multiple_of(source * block, block), block)
            values = xbuf[par, rows, cols]
            product = jnp.dot(values, wjb[par, cols, :], preferred_element_type=jnp.float32)
            wide = values.astype(jnp.float32)
            wide = wide * wide
            power = wide[:, :HD]
            for at in range(1, block // HD):
                power = power + wide[:, at * HD : (at + 1) * HD]
            if first:
                acc[:, :joined] = product
                ssq[...] = power
            else:
                acc[:, :joined] += product
                ssq[...] += power

        add(me, True)
        forward(x_args, par, h)
        waits(x_args, par, h, (1,))
        add(left, False)
        waits(x_args, par, h, (3,))
        add(right, False)
        waits(x_args, par, h, (4, 5))
        add(opposite, False)

    def attend(par, h):
        rows = pl.ds(h * half, half)
        keys = half * (h + 1)
        power = jnp.sum(ssq[...], axis=1, keepdims=True) * (1.0 / (parts * block))
        scale = lax.rsqrt(power + EPS)
        cosine = cos_ref[rows, :] * scale
        sinus = sin_ref[rows, :] * scale

        def turned(at):
            values = acc[:, at * HD : (at + 1) * HD]
            return values * cosine + pltpu.roll(values, HD // 2, 1) * sinus

        kb[rows, :] = turned(heads).astype(jnp.bfloat16)
        vb[rows, :] = (acc[:, (heads + 1) * HD : (heads + 2) * HD] * scale).astype(jnp.bfloat16)
        for head in range(heads):
            query = (turned(head) * HD ** (-0.5)).astype(jnp.bfloat16)
            scores = lax.dot_general(
                query,
                kb[:keys, :],
                (((1,), (1,)), ((), ())),
                preferred_element_type=jnp.float32,
            )
            scores = scores + bias[rows, :keys]
            top = jnp.max(scores, axis=1, keepdims=True)
            probs = jnp.exp(scores - top)
            total = jnp.sum(probs, axis=1, keepdims=True)
            mixed = jnp.dot(
                probs.astype(jnp.bfloat16), vb[:keys, :], preferred_element_type=jnp.float32
            )
            cols = pl.ds(pl.multiple_of(me * query_width + head * HD, HD), HD)
            mbuf[par, rows, cols] = (mixed / total).astype(jnp.bfloat16)
            if head == heads // 2 - 1:
                sent(0, *m_args, par, h).start()
                sent(3, *m_args, par, h).start()
                if h == 1:
                    forward(m_args, par, 0)
        sent(2, *m_args, par, h).start()
        sent(1, *m_args, par, h).start()

    def leave(par, h, layer):
        rows = pl.ds(h * half, half)
        if h == 1:
            forward(m_args, par, h)

        def term(source):
            cols = pl.ds(pl.multiple_of(source * query_width, query_width), query_width)
            return jnp.dot(
                mbuf[par, rows, cols], wob[par, cols, :], preferred_element_type=jnp.float32
            )

        acc[...] = xbuf[par, rows, own_cols].astype(jnp.float32) + term(me)
        waits(m_args, par, h, (1,))
        acc[...] += term(left)
        waits(m_args, par, h, (3,))
        acc[...] += term(right)
        waits(m_args, par, h, (4, 5))
        wait_sends(x_args, par, h)
        result = (acc[...] + term(opposite)).astype(jnp.bfloat16)

        @pl.when(layer < layers - 1)
        def _():
            xbuf[1 - par, rows, own_cols] = result
            start_own(1 - par, h)

        @pl.when(layer == layers - 1)
        def _():
            fin[rows, :] = result

    def one_layer(layer, carry):
        par = lax.rem(layer, 2)
        joined_copies, out_copies = weight_copies(layer, par)
        for copy in joined_copies:
            copy.wait()

        @pl.when(layer < layers - 1)
        def _():
            for copies_of in weight_copies(layer + 1, 1 - par):
                for copy in copies_of:
                    copy.start()

        for h in range(2):
            project(par, h)

            @pl.when(layer > 0)
            def _():
                wait_sends(m_args, 1 - par, h)

            attend(par, h)
        for copy in out_copies:
            copy.wait()
        for h in range(2):
            leave(par, h, layer)
        return carry

    lax.fori_loop(0, layers, one_layer, 0)
    last = (layers - 1) % 2

    def shared(step):
        target = lax.rem(me + step, parts)
        return pltpu.make_async_remote_copy(
            src_ref=fin.at[pl.ds(pl.multiple_of(target * token_share, token_share), token_share), :],
            dst_ref=hid.at[:, own_cols],
            send_sem=fs.at[step - 1],
            recv_sem=fr.at[step - 1],
            device_id={"mp": target},
            device_id_type=MESH,
        )

    for step in (2, 1, 3):
        shared(step).start()
    hid[:, own_cols] = fin[pl.ds(pl.multiple_of(me * token_share, token_share), token_share), :]
    for h in range(2):
        wait_sends(m_args, last, h)
    for step in (2, 1, 3):
        shared(step).wait()
    out_ref[...] = hid[...]


def decode(state, segment_ids, weights):
    length, block = state.shape
    parts = lax.axis_size("mp")
    copies = lax.axis_size(DP)
    depth = weights.shape[1]
    joined = weights.shape[2] - parts * (block // copies)
    cosine, sinus = rope_tables(length)
    dma = pltpu.SemaphoreType.DMA
    vmem = pl.BlockSpec(memory_space=pltpu.VMEM)
    return pl.pallas_call(
        decoder_kernel,
        out_shape=jax.ShapeDtypeStruct((length // parts, parts * block), jnp.bfloat16),
        in_specs=[vmem] * 5 + [pl.BlockSpec(memory_space=pl.ANY)],
        out_specs=vmem,
        scratch_shapes=[
            pltpu.VMEM((2, length, parts * block), jnp.bfloat16),
            pltpu.VMEM((2, length, parts * depth), jnp.bfloat16),
            pltpu.VMEM((2, copies * depth, joined), jnp.bfloat16),
            pltpu.VMEM((2, parts * depth, block), jnp.bfloat16),
            pltpu.VMEM((length // 2, block), jnp.float32),
            pltpu.VMEM((length // 2, HD), jnp.float32),
            pltpu.VMEM((length, HD), jnp.bfloat16),
            pltpu.VMEM((length, HD), jnp.bfloat16),
            pltpu.VMEM((length, length), jnp.float32),
            pltpu.VMEM((length, block), jnp.bfloat16),
            pltpu.VMEM((length // parts, parts * block), jnp.bfloat16),
            dma((2, 2, 6)),
            dma((2, 2, 6)),
            dma((2, 2, 6)),
            dma((2, 2, 6)),
            dma((2, copies)),
            dma((2, copies * parts)),
            dma((3,)),
            dma((3,)),
        ],
        compiler_params=pltpu.CompilerParams(
            collective_id=0, has_side_effects=True, vmem_limit_bytes=60 * 1024 * 1024
        ),
    )(segment_ids[:, None], segment_ids[None, :], cosine, sinus, state, weights)


def shards(
    text,
    patches,
    segments,
    loss_mask,
    tile_batch,
    tile_offset,
    attn_gain,
    w_query,
    w_kv,
    w_out,
    vis_gain,
    vis_bias,
    v_qkv,
    v_out,
    v_up,
    v_down,
    v_proj,
):
    section_at = lax.axis_index("section")
    parts = lax.axis_size("mp")
    copies = lax.axis_size(DP)
    copy_at = lax.axis_index(DP)
    model_width = w_query.shape[1]
    row_share = model_width // copies
    pick = lambda array: lax.dynamic_slice_in_dim(array, copy_at * row_share, row_share, 0)
    own_rows = jnp.concatenate([pick(w_query[0]), pick(w_kv[0, 0]), pick(w_kv[0, 1])], axis=1)
    own_gain = lax.dynamic_slice_in_dim(attn_gain[0], copy_at * row_share, row_share, 0)
    own_rows = (own_rows.astype(jnp.float32) * own_gain[:, None]).astype(jnp.bfloat16)
    block_width = model_width // parts
    col_share = block_width // copies
    own_out = w_out[0].reshape(w_out.shape[1], parts, copies, col_share)
    own_out = lax.dynamic_slice_in_dim(own_out, copy_at, 1, 2)[:, :, 0]
    own_out = lax.all_to_all(
        jnp.moveaxis(own_out, 1, 0), "mp", split_axis=0, concat_axis=0, tiled=True
    )
    own_out = jnp.moveaxis(own_out, 0, 1).reshape(w_out.shape[1], parts * col_share)
    own = jnp.concatenate([own_rows, own_out], axis=1)
    weights = lax.all_gather(own, SECTION_DP)
    small = jnp.concatenate([v_qkv[0], v_qkv[1], v_qkv[2], v_out.T, v_up, v_down.T], axis=1)
    sections = lax.axis_size("section")
    batch_all = tile_batch[0].reshape(sections, -1)
    offset_all = tile_offset[0].reshape(sections, -1)
    own_batch = lax.dynamic_slice_in_dim(batch_all, section_at, 1, 0)
    own_batch = jnp.repeat(own_batch, POOL, axis=1)
    starts = jnp.max(jnp.where(batch_all == section_at, offset_all, -POOL), axis=1)
    place = jnp.repeat(starts, POOL) + jnp.tile(jnp.arange(POOL, dtype=jnp.int32), sections)
    patches, own = lax.optimization_barrier((patches, own))
    state, token_weight = encode(
        patches,
        vis_gain,
        vis_bias,
        text[0],
        loss_mask,
        own_batch,
        place[None, :],
        small,
        v_proj,
    )
    hidden = decode(state, segments[0, 0], weights)
    return (hidden[None], token_weight)


def solution(mesh):
    split = Mesh(
        mesh.devices.reshape(mesh.shape["section"], 4, 2, mesh.shape["mp"]),
        ("section", "dp_0", "dp_1", "mp"),
    )
    return jax.shard_map(
        shards,
        mesh=split,
        in_specs=(
            P("section", DP_MP, None),
            P(SECTION_DP, None),
            P("section", DP, None),
            P("section", DP_MP),
            P(DP, None),
            P(DP, None),
            P("section", None),
            P("section", None, "mp"),
            P("section", None, None, "mp"),
            P("section", "mp", None),
            P(),
            P(),
            P(None, SECTION_DP, "mp"),
            P("mp", SECTION_DP),
            P(SECTION_DP, "mp"),
            P("mp", SECTION_DP),
            P(SECTION_DP, "mp"),
        ),
        out_specs=(P("section", DP_MP, None), P("section", DP_MP)),
        check_vma=False,
    )
```

```python
import jax
import jax.numpy as jnp
from jax import lax
from jax.experimental import pallas as pl
from jax.experimental.pallas import tpu as pltpu
from jax.sharding import Mesh
from jax.sharding import PartitionSpec as P

HD = 128
VHD = 64
GRID = 16
PATCH = 256
POOL = 64
SECTION_DP = ("section", "dp_0", "dp_1")
SECTION_DP_MP = ("section", "dp_0", "dp_1", "mp")
DP = ("dp_0", "dp_1")
DP_MP = ("dp_0", "dp_1", "mp")


EPS = 1e-05
ROPE_BASE = 500000.0
BLOCKED = -1e30
MESH = pl.DeviceIdType.MESH


def rope_tables(length):
    half_width = HD // 2
    freqs = ROPE_BASE ** (-2.0 * jnp.arange(half_width, dtype=jnp.float32) / HD)
    angles = jnp.arange(length, dtype=jnp.float32)[:, None] * freqs[None, :]
    cosine, sinus = jnp.cos(angles), jnp.sin(angles)
    return (
        jnp.concatenate([cosine, cosine], axis=1),
        jnp.concatenate([-sinus, sinus], axis=1),
    )


def vision_kernel(
    patches_ref,
    gain_ref,
    bias_ref,
    text_ref,
    mask_ref,
    own_ref,
    place_ref,
    small_ref,
    proj_ref,
    state_ref,
    weight_ref,
    sm,
    pj,
    joined,
    mix,
    part,
    rsb,
    res,
    n2,
    pooled,
    blk,
    arrived,
    txt,
    cbuf,
    gs,
    gr,
    xs,
    xr,
    zs,
    zr,
    ts,
    tr,
    cs,
    cr,
    loc,
    whole,
    hs,
    hr,
):
    parts = 4
    z, y, c, me = (lax.axis_index(name) for name in ("section", "dp_0", "dp_1", "mp"))
    rows, width = patches_ref.shape
    tiles = rows // PATCH
    share = PATCH // parts
    local = width // parts
    hidden = small_ref.shape[1] // 2 - 2 * local
    block = text_ref.shape[1] // parts
    token_share = text_ref.shape[0]
    pool_share = POOL // parts

    def place_of(core, first, second):
        return first * (8 - 6 * core) + second * (2 + 6 * core) + core

    a, b = z * (1 - c) + y * c, y * (1 - c) + z * c
    pa, pb = z * c + y * (1 - c), y * c + z * (1 - c)

    def along_a(step):
        return {"section": lax.rem(z + (1 - c) * step, 4), "dp_0": lax.rem(y + c * step, 4)}

    def along_b(step):
        return {"section": lax.rem(z + c * step, 4), "dp_0": lax.rem(y + (1 - c) * step, 4)}

    def along_x(step):
        return {"mp": lax.rem(me + step, parts)}

    partner = {"dp_1": 1 - c}
    full, own_piece = (sm, pj), (small_ref, proj_ref)

    def remote(src, dst, send, recv, target):
        return pltpu.make_async_remote_copy(
            src_ref=src,
            dst_ref=dst,
            send_sem=send,
            recv_sem=recv,
            device_id=target,
            device_id_type=MESH,
        )

    def region(arr, core, first, second):
        count = own_piece[arr].shape[0]
        at = place_of(core, lax.rem(first, 4), lax.rem(second, 4))
        return full[arr].at[pl.ds(pl.multiple_of(at * count, count), count), :]

    def share_out(arr, kind, ra, rb, target):
        dst = region(arr, c, a + ra, b + rb)
        src = own_piece[arr] if (ra, rb) == (0, 0) else dst
        return remote(src, dst, gs.at[arr, kind], gr.at[arr, kind], target)

    started = ([], [])

    def give(arr, kind, ra, rb, target):
        copy = share_out(arr, kind, ra, rb, target)
        copy.start()
        started[arr].append(copy)

    def take(arr, kind, ra, rb):
        share_out(arr, kind, ra, rb, partner).wait_recv()

    def to_both(arr, ra):
        give(arr, 3 + ra, ra, 0, along_b(1))
        give(arr, 7 + ra, ra, 0, along_b(3))
        give(arr, 15 + ra * 4, ra, 0, partner)

    def gather_start(arr):
        give(arr, 0, 0, 0, along_a(1))
        give(arr, 1, 0, 0, along_a(3))
        to_both(arr, 0)
        pltpu.make_async_copy(own_piece[arr], region(arr, c, a, b), loc.at[arr]).start()

    def gather_a(arr):
        take(arr, 0, 3, 0)
        if arr == 0:
            give(arr, 2, 3, 0, along_a(1))
        to_both(arr, 3)
        take(arr, 1, 1, 0)
        if arr == 1:
            give(arr, 2, 1, 0, along_a(3))
        to_both(arr, 1)
        take(arr, 2, 2, 0)
        to_both(arr, 2)

    def gather_b(arr):
        for ra in (0, 3, 1, 2):
            take(arr, 3 + ra, ra, 3)
            if ra < 2:
                give(arr, 11 + ra, ra, 3, along_b(1))
            give(arr, 15 + ra * 4 + 3, ra, 3, partner)
            take(arr, 7 + ra, ra, 1)
            if ra >= 2:
                give(arr, 11 + ra, ra, 1, along_b(3))
            give(arr, 15 + ra * 4 + 1, ra, 1, partner)

    def gather_b2(arr):
        for ra in (0, 3, 1, 2):
            take(arr, 11 + ra, ra, 2)
            give(arr, 15 + ra * 4 + 2, ra, 2, partner)

    def gather_end(arr):
        for ra in range(4):
            for rb in range(4):
                kind = 15 + ra * 4 + rb
                dst = region(arr, 1 - c, pa + ra, pb + rb)
                remote(dst, dst, gs.at[arr, kind], gr.at[arr, kind], partner).wait_recv()
        pltpu.make_async_copy(own_piece[arr], region(arr, c, a, b), loc.at[arr]).wait()

    def count_copy(stage, step):
        name = ("mp", "dp_1", "dp_0", "section")[stage]
        at = (me, c, y, z)[stage]
        size = (4, 2, 4, 4)[stage]
        return remote(
            cbuf.at[stage, 3],
            cbuf.at[stage, step - 1],
            cs.at[stage, step - 1],
            cr.at[stage, step - 1],
            {name: lax.rem(at + step, size)},
        )

    def count_steps(stage):
        return (1,) if stage == 1 else (1, 2, 3)

    def count_send(stage):
        for step in count_steps(stage):
            count_copy(stage, step).start()

    def count_sum(stage):
        total = cbuf[stage, 3]
        for step in count_steps(stage):
            count_copy(stage, step).wait()
            total = total + cbuf[stage, step - 1]
        return total

    def text_copy(step):
        target = lax.rem(me + step, parts)
        return remote(
            text_ref.at[:, pl.ds(pl.multiple_of(target * block, block), block)],
            txt.at[pl.ds(pl.multiple_of(me * token_share, token_share), token_share), :],
            ts.at[step - 1],
            tr.at[step - 1],
            along_x(step),
        )

    def scatter_copy(stage, tile, step):
        target = lax.rem(me + step, parts)
        return remote(
            part.at[stage, tile, pl.ds(pl.multiple_of(target * share, share), share), :],
            rsb.at[stage, tile, step - 1],
            xs.at[2 * stage, tile, step - 1],
            xr.at[2 * stage, tile, step - 1],
            along_x(step),
        )

    def spread_copy(stage, tile, step):
        if stage == 0:
            ref = n2.at[tile, pl.ds(pl.multiple_of(me * share, share), share), :]
        else:
            ref = pooled.at[
                pl.ds(pl.multiple_of(tile * POOL + me * pool_share, pool_share), pool_share), :
            ]
        return remote(
            ref, ref, xs.at[2 * stage + 1, tile, step - 1], xr.at[2 * stage + 1, tile, step - 1], along_x(step)
        )

    def normed(wide, at):
        center = wide - jnp.mean(wide, axis=1, keepdims=True)
        spread = jnp.mean(center * center, axis=1, keepdims=True)
        scaled = center * lax.rsqrt(spread + EPS) * gain_ref[at : at + 1, :]
        return (scaled + bias_ref[at : at + 1, :]).astype(jnp.bfloat16)

    def own_sum(stage, tile):
        mine = pl.ds(pl.multiple_of(me * share, share), share)
        total = part[stage, tile, mine, :].astype(jnp.float32)
        for step in (1, 3, 2):
            scatter_copy(stage, tile, step).wait()
            total = total + rsb[stage, tile, step - 1].astype(jnp.float32)
        return total

    barrier = pltpu.get_barrier_semaphore()
    others = [{"section": lax.rem(z + step, 4)} for step in (1, 2, 3)]
    others += [{"dp_0": lax.rem(y + step, 4)} for step in (1, 2, 3)]
    others += [along_x(step) for step in (1, 2, 3)] + [partner]
    for target in others:
        pl.semaphore_signal(barrier, inc=1, device_id=target, device_id_type=MESH)
    mask = mask_ref[...].astype(jnp.float32)
    cbuf[0, 3] = jnp.broadcast_to(jnp.sum(mask, axis=1, keepdims=True), cbuf.shape[2:])
    pl.semaphore_wait(barrier, len(others))
    gather_start(0)
    gather_start(1)
    for step in (1, 3, 2):
        text_copy(step).start()
    count_send(0)
    own_rows = pl.ds(pl.multiple_of(me * token_share, token_share), token_share)
    txt[own_rows, :] = text_ref[:, pl.ds(pl.multiple_of(me * block, block), block)]
    first = normed(patches_ref[...].astype(jnp.float32), 0)
    gather_a(0)
    gather_a(1)
    gather_b(0)
    gather_b2(0)
    cbuf[1, 3] = count_sum(0)
    count_send(1)
    gather_end(0)
    joined[...] = jnp.dot(first, sm[:, : 3 * local], preferred_element_type=jnp.float32)
    low = lax.broadcasted_iota(jnp.int32, (PATCH, 2 * VHD), 1) < VHD

    def attend(tile):
        at = pl.ds(tile * PATCH, PATCH)
        for pair in range(local // (2 * VHD)):
            start = pair * 2 * VHD
            query = joined[at, start : start + 2 * VHD]
            keyed = joined[at, local + start : local + start + 2 * VHD].astype(jnp.bfloat16)
            valued = joined[at, 2 * local + start : 2 * local + start + 2 * VHD]
            valued = valued.astype(jnp.bfloat16)
            found = []
            for side in (low, jnp.logical_not(low)):
                masked = jnp.where(side, query, 0.0).astype(jnp.bfloat16)
                scores = lax.dot_general(
                    masked, keyed, (((1,), (1,)), ((), ())), preferred_element_type=jnp.float32
                )
                scores = scores * VHD ** (-0.5)
                probs = jnp.exp(scores - jnp.max(scores, axis=1, keepdims=True))
                total = jnp.sum(probs, axis=1, keepdims=True)
                product = jnp.dot(
                    probs.astype(jnp.bfloat16), valued, preferred_element_type=jnp.float32
                )
                found.append(product / total)
            mix[at, start : start + 2 * VHD] = jnp.where(low, *found).astype(jnp.bfloat16)
        partial_sum = lax.dot_general(
            mix[at, :],
            sm[:, 3 * local : 4 * local],
            (((1,), (1,)), ((), ())),
            preferred_element_type=jnp.float32,
        )
        part[0, tile] = partial_sum.astype(jnp.bfloat16)
        for step in (1, 3, 2):
            scatter_copy(0, tile, step).start()

    def middle(tile):
        mine = pl.ds(pl.multiple_of(tile * PATCH + me * share, share), share)
        total = patches_ref[mine, :].astype(jnp.float32) + own_sum(0, tile)
        kept = total.astype(jnp.bfloat16)
        res[tile] = kept
        rows_here = pl.ds(pl.multiple_of(me * share, share), share)
        n2[tile, rows_here, :] = normed(kept.astype(jnp.float32), 1)
        for step in (1, 3, 2):
            spread_copy(0, tile, step).start()

    def expand(tile):
        for step in (1, 3, 2):
            spread_copy(0, tile, step).wait()
        inner = jnp.dot(
            n2[tile],
            sm[:, 4 * local : 4 * local + hidden],
            preferred_element_type=jnp.float32,
        )
        inner = (0.5 * inner * (1.0 + lax.erf(inner * 0.5**0.5))).astype(jnp.bfloat16)
        partial_sum = lax.dot_general(
            inner,
            sm[:, 4 * local + hidden :],
            (((1,), (1,)), ((), ())),
            preferred_element_type=jnp.float32,
        )
        part[1, tile] = partial_sum.astype(jnp.bfloat16)
        for step in (1, 3, 2):
            scatter_copy(1, tile, step).start()

    row_at = lax.broadcasted_iota(jnp.int32, (share, share), 0)
    col_at = lax.broadcasted_iota(jnp.int32, (share, share), 1)
    quad, token = row_at // pool_share, row_at % pool_share
    side = GRID // 2
    origin = 2 * GRID * (token // side) + GRID * (quad // 2) + 2 * (token % side) + quad % 2
    shuffle = (col_at == origin).astype(jnp.float32).astype(jnp.bfloat16)

    def pool(tile):
        kept = (res[tile].astype(jnp.float32) + own_sum(1, tile)).astype(jnp.bfloat16)
        moved = jnp.dot(shuffle, kept, preferred_element_type=jnp.float32).astype(jnp.bfloat16)
        mine = pl.ds(pl.multiple_of(tile * POOL + me * pool_share, pool_share), pool_share)
        for at in range(4):
            pooled[mine, at * width : (at + 1) * width] = moved[
                at * pool_share : (at + 1) * pool_share, :
            ]
        for step in (1, 3, 2):
            spread_copy(1, tile, step).start()

    attend(0)
    gather_b(1)
    attend(1)
    middle(0)
    gather_b2(1)
    middle(1)
    cbuf[2, 3] = count_sum(1)
    count_send(2)
    for tile in range(tiles):
        expand(tile)
    for tile in range(tiles):
        pool(tile)
    cbuf[3, 3] = count_sum(2)
    count_send(3)
    gather_end(1)
    for tile in range(tiles):
        for step in (1, 3, 2):
            spread_copy(1, tile, step).wait()
    image = jnp.dot(pooled[...], pj[...], preferred_element_type=jnp.float32).astype(jnp.bfloat16)
    send_row = lax.broadcasted_iota(jnp.int32, (4 * POOL, tiles * POOL), 0)
    send_col = lax.broadcasted_iota(jnp.int32, (4 * POOL, tiles * POOL), 1)
    chosen = (own_ref[...] == send_row // POOL) & (send_row % POOL == send_col % POOL)
    chosen = chosen.astype(jnp.float32).astype(jnp.bfloat16)
    blk[...] = jnp.dot(chosen, image, preferred_element_type=jnp.float32).astype(jnp.bfloat16)

    def home_copy(step):
        target = lax.rem(z + step, 4)
        return remote(
            blk.at[pl.ds(pl.multiple_of(target * POOL, POOL), POOL), :],
            arrived.at[pl.ds(pl.multiple_of(z * POOL, POOL), POOL), :],
            zs.at[step - 1],
            zr.at[step - 1],
            {"section": target},
        )

    for step in (2, 1, 3):
        home_copy(step).start()
    here = pl.ds(pl.multiple_of(z * POOL, POOL), POOL)
    arrived[here, :] = blk[here, :]
    count = count_sum(3)
    scaling = float(4 * 8 * parts * token_share)
    weight_ref[...] = mask * scaling / count[:1, :]
    length = state_ref.shape[0]
    picked = lax.broadcasted_iota(jnp.int32, (length, 4 * POOL), 0) == place_ref[...]
    picked = picked.astype(jnp.float32)
    covered = jnp.max(picked, axis=1, keepdims=True) > 0.5
    for step in (1, 3, 2):
        text_copy(step).wait()
    for copies_of in started:
        for copy in copies_of:
            copy.wait_send()
    for step in (1, 3, 2):
        home_copy(step).wait()
    placed = jnp.dot(
        picked.astype(jnp.bfloat16), arrived[...], preferred_element_type=jnp.float32
    )
    half = block // 2

    def state_copy(kind, incoming):
        if incoming:
            back = (3, 3, 1, 1, 2, 2)[kind]
        else:
            back = (0, 0, 0, 0, 3, 1)[kind]
        at = lax.rem(me + back, parts) * block + (0, 1, 1, 0, 0, 1)[kind] * half
        ref = whole.at[:, pl.ds(pl.multiple_of(at, half), half)]
        return remote(ref, ref, hs.at[kind], hr.at[kind], along_x((1, 1, 3, 3, 1, 3)[kind]))

    first_state = jnp.where(covered, placed, txt[...].astype(jnp.float32)).astype(jnp.bfloat16)
    whole[:, pl.ds(pl.multiple_of(me * block, block), block)] = first_state
    for kind in (0, 2, 1, 3):
        state_copy(kind, False).start()
    state_copy(0, True).wait_recv()
    state_copy(4, False).start()
    state_copy(2, True).wait_recv()
    state_copy(5, False).start()
    for kind in (1, 3, 4, 5):
        state_copy(kind, True).wait_recv()
    for kind in range(6):
        state_copy(kind, False).wait_send()
    state_ref[...] = whole[...]


def encode(patches, vis_gain, vis_bias, text, mask, own, place, small, proj):
    rows, width = patches.shape
    tiles = rows // PATCH
    block = text.shape[1] // 4
    length = text.shape[0] * 4
    share = PATCH // 4
    dma = pltpu.SemaphoreType.DMA
    vmem = pl.BlockSpec(memory_space=pltpu.VMEM)
    bf16 = jnp.bfloat16
    return pl.pallas_call(
        vision_kernel,
        out_shape=(
            jax.ShapeDtypeStruct((length, 4 * block), bf16),
            jax.ShapeDtypeStruct(mask.shape, jnp.float32),
        ),
        in_specs=[vmem] * 9,
        out_specs=(vmem, vmem),
        scratch_shapes=[
            pltpu.VMEM((small.shape[0] * 32, small.shape[1]), bf16),
            pltpu.VMEM((proj.shape[0] * 32, proj.shape[1]), bf16),
            pltpu.VMEM((rows, 3 * width // 4), jnp.float32),
            pltpu.VMEM((rows, width // 4), bf16),
            pltpu.VMEM((2, tiles, PATCH, width), bf16),
            pltpu.VMEM((2, tiles, 3, share, width), bf16),
            pltpu.VMEM((tiles, share, width), bf16),
            pltpu.VMEM((tiles, PATCH, width), bf16),
            pltpu.VMEM((tiles * POOL, 4 * width), bf16),
            pltpu.VMEM((4 * POOL, block), bf16),
            pltpu.VMEM((4 * POOL, block), bf16),
            pltpu.VMEM((length, block), bf16),
            pltpu.VMEM((4, 4, 8, 128), jnp.float32),
            dma((2, 31)),
            dma((2, 31)),
            dma((4, tiles, 3)),
            dma((4, tiles, 3)),
            dma((3,)),
            dma((3,)),
            dma((3,)),
            dma((3,)),
            dma((4, 3)),
            dma((4, 3)),
            dma((2,)),
            pltpu.VMEM((length, 4 * block), bf16),
            dma((6,)),
            dma((6,)),
        ],
        compiler_params=pltpu.CompilerParams(
            collective_id=1, has_side_effects=True, vmem_limit_bytes=56 * 1024 * 1024
        ),
    )(patches, vis_gain, vis_bias, text, mask, own, place, small, proj)


def decoder_kernel(
    seg_col,
    seg_row,
    cos_ref,
    sin_ref,
    s0_ref,
    w_any,
    out_ref,
    xbuf,
    mbuf,
    wjb,
    wob,
    acc,
    ssq,
    kb,
    vb,
    bias,
    fin,
    hid,
    xs,
    xr,
    ms,
    mr,
    js,
    os,
    fs,
    fr,
    rs,
):
    parts = 4
    layers = 4
    copies = w_any.shape[0] // layers
    length = s0_ref.shape[0]
    block = s0_ref.shape[1] // parts
    half = length // 2
    joined = wjb.shape[2]
    query_width = wob.shape[1] // parts
    heads = query_width // HD
    depth = w_any.shape[1]
    col_share = wob.shape[2] // copies
    token_share = length // parts
    me = lax.axis_index("mp")
    right, opposite, left = (lax.rem(me + step, parts) for step in (1, 2, 3))

    def weight_copies(layer, par):
        found = []
        for d in range(copies):
            found.append(
                pltpu.make_async_copy(
                    w_any.at[layer * copies + d, :, pl.ds(0, joined)],
                    wjb.at[par, pl.ds(d * depth, depth), :],
                    js.at[par, d],
                )
            )
        for d in range(copies):
            for part in range(parts):
                found.append(
                    pltpu.make_async_copy(
                        w_any.at[
                            layer * copies + d, :, pl.ds(joined + part * col_share, col_share)
                        ],
                        wob.at[par, pl.ds(part * depth, depth), pl.ds(d * col_share, col_share)],
                        os.at[par, d * parts + part],
                    )
                )
        return found[:copies], found[copies:]

    def piece(buf, width, sends, recvs, par, h, kind, source, half_at, target):
        cols = pl.ds(pl.multiple_of(source * width + half_at * (width // 2), width // 2), width // 2)
        ref = buf.at[par, pl.ds(h * half, half), cols]
        return pltpu.make_async_remote_copy(
            src_ref=ref,
            dst_ref=ref,
            send_sem=sends.at[par, h, kind],
            recv_sem=recvs.at[par, h, kind],
            device_id={"mp": target},
            device_id_type=MESH,
        )

    def sent(kind, buf, width, sends, recvs, par, h):
        source, half_at, target = (
            (me, 0, right),
            (me, 1, right),
            (me, 1, left),
            (me, 0, left),
            (left, 0, right),
            (right, 1, left),
        )[kind]
        return piece(buf, width, sends, recvs, par, h, kind, source, half_at, target)

    def landed(kind, buf, width, sends, recvs, par, h):
        source, half_at = (
            (left, 0),
            (left, 1),
            (right, 1),
            (right, 0),
            (opposite, 0),
            (opposite, 1),
        )[kind]
        return piece(buf, width, sends, recvs, par, h, kind, source, half_at, right)

    x_args = (xbuf, block, xs, xr)
    m_args = (mbuf, query_width, ms, mr)

    def forward(args, par, h):
        landed(0, *args, par, h).wait_recv()
        sent(4, *args, par, h).start()
        landed(2, *args, par, h).wait_recv()
        sent(5, *args, par, h).start()

    def waits(args, par, h, kinds):
        for kind in kinds:
            landed(kind, *args, par, h).wait_recv()

    def wait_sends(args, par, h):
        for kind in range(6):
            sent(kind, *args, par, h).wait_send()

    def start_own(par, h):
        for kind in (0, 2, 1, 3):
            sent(kind, *x_args, par, h).start()

    first_joined, first_out = weight_copies(0, 0)
    for copy in first_joined + first_out:
        copy.start()
    barrier = pltpu.get_barrier_semaphore()
    for target in (right, opposite, left):
        pl.semaphore_signal(barrier, inc=1, device_id={"mp": target}, device_id_type=MESH)
    own_cols = pl.ds(pl.multiple_of(me * block, block), block)
    ready = pltpu.make_async_copy(s0_ref, xbuf.at[0], rs.at[0])
    ready.start()
    rows_at = lax.broadcasted_iota(jnp.int32, (length, length), 0)
    cols_at = lax.broadcasted_iota(jnp.int32, (length, length), 1)
    allowed = (seg_col[...] == seg_row[...]) & (cols_at <= rows_at)
    bias[...] = jnp.where(allowed, 0.0, BLOCKED)
    pl.semaphore_wait(barrier, 3)
    ready.wait()

    def project(par, h, layer):
        rows = pl.ds(h * half, half)

        def add(source, first):
            cols = pl.ds(pl.multiple_of(source * block, block), block)
            values = xbuf[par, rows, cols]
            product = jnp.dot(values, wjb[par, cols, :], preferred_element_type=jnp.float32)
            wide = values.astype(jnp.float32)
            wide = wide * wide
            power = wide[:, :HD]
            for at in range(1, block // HD):
                power = power + wide[:, at * HD : (at + 1) * HD]
            if first:
                acc[:, :joined] = product
                ssq[...] = power
            else:
                acc[:, :joined] += product
                ssq[...] += power

        def arrive(step):
            @pl.when(layer > 0)
            def _():
                step()

        add(me, True)
        if h == 1:
            arrive(lambda: forward(x_args, par, h))
        arrive(lambda: waits(x_args, par, h, (1,)))
        add(left, False)
        arrive(lambda: waits(x_args, par, h, (3,)))
        add(right, False)
        if h == 1:
            forward(m_args, par, 0)
        arrive(lambda: waits(x_args, par, h, (4, 5)))
        add(opposite, False)

    def attend(par, h):
        rows = pl.ds(h * half, half)
        keys = half * (h + 1)
        power = jnp.sum(ssq[...], axis=1, keepdims=True) * (1.0 / (parts * block))
        scale = lax.rsqrt(power + EPS)
        cosine = cos_ref[rows, :] * scale
        sinus = sin_ref[rows, :] * scale

        def turned(at):
            values = acc[:, at * HD : (at + 1) * HD]
            return values * cosine + pltpu.roll(values, HD // 2, 1) * sinus

        kb[rows, :] = turned(heads).astype(jnp.bfloat16)
        vb[rows, :] = (acc[:, (heads + 1) * HD : (heads + 2) * HD] * scale).astype(jnp.bfloat16)
        for head in range(heads):
            query = (turned(head) * HD ** (-0.5)).astype(jnp.bfloat16)
            scores = lax.dot_general(
                query,
                kb[:keys, :],
                (((1,), (1,)), ((), ())),
                preferred_element_type=jnp.float32,
            )
            scores = scores + bias[rows, :keys]
            top = jnp.max(scores, axis=1, keepdims=True)
            probs = jnp.exp(scores - top)
            total = jnp.sum(probs, axis=1, keepdims=True)
            mixed = jnp.dot(
                probs.astype(jnp.bfloat16), vb[:keys, :], preferred_element_type=jnp.float32
            )
            cols = pl.ds(pl.multiple_of(me * query_width + head * HD, HD), HD)
            mbuf[par, rows, cols] = (mixed / total).astype(jnp.bfloat16)
            if head == heads // 2 - 1:
                sent(0, *m_args, par, h).start()
                sent(3, *m_args, par, h).start()
        sent(2, *m_args, par, h).start()
        sent(1, *m_args, par, h).start()

    def leave(par, h, layer):
        rows = pl.ds(h * half, half)

        def term(source):
            cols = pl.ds(pl.multiple_of(source * query_width, query_width), query_width)
            return jnp.dot(
                mbuf[par, rows, cols], wob[par, cols, :], preferred_element_type=jnp.float32
            )

        acc[...] = xbuf[par, rows, own_cols].astype(jnp.float32) + term(me)
        waits(m_args, par, h, (1,))
        acc[...] += term(left)
        waits(m_args, par, h, (3,))
        acc[...] += term(right)
        waits(m_args, par, h, (4, 5))

        @pl.when(layer > 0)
        def _():
            wait_sends(x_args, par, h)

        result = (acc[...] + term(opposite)).astype(jnp.bfloat16)
        if h == 0:
            forward(m_args, par, 1)

        @pl.when(layer < layers - 1)
        def _():
            xbuf[1 - par, rows, own_cols] = result
            if h == 1:
                forward(x_args, 1 - par, 0)
            start_own(1 - par, h)

        @pl.when(layer == layers - 1)
        def _():
            fin[rows, :] = result

    def one_layer(layer, carry):
        par = lax.rem(layer, 2)
        joined_copies, out_copies = weight_copies(layer, par)
        for copy in joined_copies:
            copy.wait()

        @pl.when(layer < layers - 1)
        def _():
            for copies_of in weight_copies(layer + 1, 1 - par):
                for copy in copies_of:
                    copy.start()

        for h in range(2):
            project(par, h, layer)

            @pl.when(layer > 0)
            def _():
                wait_sends(m_args, 1 - par, h)

            attend(par, h)
        for copy in out_copies:
            copy.wait()
        for h in range(2):
            leave(par, h, layer)
        return carry

    lax.fori_loop(0, layers, one_layer, 0)
    last = (layers - 1) % 2

    def shared(step):
        target = lax.rem(me + step, parts)
        return pltpu.make_async_remote_copy(
            src_ref=fin.at[pl.ds(pl.multiple_of(target * token_share, token_share), token_share), :],
            dst_ref=hid.at[:, own_cols],
            send_sem=fs.at[step - 1],
            recv_sem=fr.at[step - 1],
            device_id={"mp": target},
            device_id_type=MESH,
        )

    for step in (2, 1, 3):
        shared(step).start()
    hid[:, own_cols] = fin[pl.ds(pl.multiple_of(me * token_share, token_share), token_share), :]
    for h in range(2):
        wait_sends(m_args, last, h)
    for step in (2, 1, 3):
        shared(step).wait()
    out_ref[...] = hid[...]


def decode(state, segment_ids, weights):
    parts = lax.axis_size("mp")
    length, block = state.shape[0], state.shape[1] // parts
    copies = lax.axis_size(DP)
    depth = weights.shape[1]
    joined = weights.shape[2] - parts * (block // copies)
    cosine, sinus = rope_tables(length)
    dma = pltpu.SemaphoreType.DMA
    vmem = pl.BlockSpec(memory_space=pltpu.VMEM)
    return pl.pallas_call(
        decoder_kernel,
        out_shape=jax.ShapeDtypeStruct((length // parts, parts * block), jnp.bfloat16),
        in_specs=[vmem] * 4 + [pl.BlockSpec(memory_space=pl.ANY)] * 2,
        out_specs=vmem,
        scratch_shapes=[
            pltpu.VMEM((2, length, parts * block), jnp.bfloat16),
            pltpu.VMEM((2, length, parts * depth), jnp.bfloat16),
            pltpu.VMEM((2, copies * depth, joined), jnp.bfloat16),
            pltpu.VMEM((2, parts * depth, block), jnp.bfloat16),
            pltpu.VMEM((length // 2, block), jnp.float32),
            pltpu.VMEM((length // 2, HD), jnp.float32),
            pltpu.VMEM((length, HD), jnp.bfloat16),
            pltpu.VMEM((length, HD), jnp.bfloat16),
            pltpu.VMEM((length, length), jnp.float32),
            pltpu.VMEM((length, block), jnp.bfloat16),
            pltpu.VMEM((length // parts, parts * block), jnp.bfloat16),
            dma((2, 2, 6)),
            dma((2, 2, 6)),
            dma((2, 2, 6)),
            dma((2, 2, 6)),
            dma((2, copies)),
            dma((2, copies * parts)),
            dma((3,)),
            dma((3,)),
            dma((1,)),
        ],
        compiler_params=pltpu.CompilerParams(
            collective_id=0, has_side_effects=True, vmem_limit_bytes=60 * 1024 * 1024
        ),
    )(segment_ids[:, None], segment_ids[None, :], cosine, sinus, state, weights)


def shards(
    text,
    patches,
    segments,
    loss_mask,
    tile_batch,
    tile_offset,
    attn_gain,
    w_query,
    w_kv,
    w_out,
    vis_gain,
    vis_bias,
    v_qkv,
    v_out,
    v_up,
    v_down,
    v_proj,
):
    section_at = lax.axis_index("section")
    parts = lax.axis_size("mp")
    copies = lax.axis_size(DP)
    copy_at = lax.axis_index(DP)
    model_width = w_query.shape[1]
    row_share = model_width // copies
    pick = lambda array: lax.dynamic_slice_in_dim(array, copy_at * row_share, row_share, 0)
    own_rows = jnp.concatenate([pick(w_query[0]), pick(w_kv[0, 0]), pick(w_kv[0, 1])], axis=1)
    own_gain = lax.dynamic_slice_in_dim(attn_gain[0], copy_at * row_share, row_share, 0)
    own_rows = (own_rows.astype(jnp.float32) * own_gain[:, None]).astype(jnp.bfloat16)
    block_width = model_width // parts
    col_share = block_width // copies
    own_out = w_out[0].reshape(w_out.shape[1], parts, copies, col_share)
    own_out = lax.dynamic_slice_in_dim(own_out, copy_at, 1, 2)[:, :, 0]
    own_out = lax.all_to_all(
        jnp.moveaxis(own_out, 1, 0), "mp", split_axis=0, concat_axis=0, tiled=True
    )
    own_out = jnp.moveaxis(own_out, 0, 1).reshape(w_out.shape[1], parts * col_share)
    own = jnp.concatenate([own_rows, own_out], axis=1)
    own, v_out, v_down = lax.optimization_barrier((own, v_out, v_down))
    small = jnp.concatenate([v_qkv[0], v_qkv[1], v_qkv[2], v_out.T, v_up, v_down.T], axis=1)
    sections = lax.axis_size("section")
    batch_all = tile_batch[0].reshape(sections, -1)
    offset_all = tile_offset[0].reshape(sections, -1)
    own_batch = lax.dynamic_slice_in_dim(batch_all, section_at, 1, 0)
    own_batch = jnp.repeat(own_batch, POOL, axis=1)
    starts = jnp.max(jnp.where(batch_all == section_at, offset_all, -POOL), axis=1)
    place = jnp.repeat(starts, POOL) + jnp.tile(jnp.arange(POOL, dtype=jnp.int32), sections)
    weights = lax.all_gather(own, SECTION_DP)
    state, token_weight = encode(
        patches,
        vis_gain,
        vis_bias,
        text[0],
        loss_mask,
        own_batch,
        place[None, :],
        small,
        v_proj,
    )
    hidden = decode(state, segments[0, 0], weights)
    return (hidden[None], token_weight)


def solution(mesh):
    split = Mesh(
        mesh.devices.reshape(mesh.shape["section"], 4, 2, mesh.shape["mp"]),
        ("section", "dp_0", "dp_1", "mp"),
    )
    return jax.shard_map(
        shards,
        mesh=split,
        in_specs=(
            P("section", DP_MP, None),
            P(SECTION_DP, None),
            P("section", DP, None),
            P("section", DP_MP),
            P(DP, None),
            P(DP, None),
            P("section", None),
            P("section", None, "mp"),
            P("section", None, None, "mp"),
            P("section", "mp", None),
            P(),
            P(),
            P(None, SECTION_DP, "mp"),
            P("mp", SECTION_DP),
            P(SECTION_DP, "mp"),
            P("mp", SECTION_DP),
            P(SECTION_DP, "mp"),
        ),
        out_specs=(P("section", DP_MP, None), P("section", DP_MP)),
        check_vma=False,
    )
```

```python
import jax
import jax.numpy as jnp
from jax import lax
from jax.experimental import pallas as pl
from jax.experimental.pallas import tpu as pltpu
from jax.sharding import Mesh
from jax.sharding import PartitionSpec as P

HD = 128
VHD = 64
GRID = 16
PATCH = 256
POOL = 64
SECTION_DP = ("section", "dp_0", "dp_1")
SECTION_DP_MP = ("section", "dp_0", "dp_1", "mp")
DP = ("dp_0", "dp_1")
DP_MP = ("dp_0", "dp_1", "mp")


EPS = 1e-05
ROPE_BASE = 500000.0
BLOCKED = -1e30
MESH = pl.DeviceIdType.MESH


def rope_tables(length):
    half_width = HD // 2
    freqs = ROPE_BASE ** (-2.0 * jnp.arange(half_width, dtype=jnp.float32) / HD)
    angles = jnp.arange(length, dtype=jnp.float32)[:, None] * freqs[None, :]
    cosine, sinus = jnp.cos(angles), jnp.sin(angles)
    return (
        jnp.concatenate([cosine, cosine], axis=1),
        jnp.concatenate([-sinus, sinus], axis=1),
    )


def vision_kernel(
    patches_ref,
    gain_ref,
    bias_ref,
    text_ref,
    mask_ref,
    own_ref,
    place_ref,
    small_ref,
    proj_ref,
    state_ref,
    weight_ref,
    sm,
    pj,
    joined,
    mix,
    part,
    rsb,
    res,
    n2,
    pooled,
    blk,
    arrived,
    images,
    cbuf,
    gs,
    gr,
    xs,
    xr,
    zs,
    zr,
    ts,
    tr,
    cs,
    cr,
    loc,
    whole,
    hs,
    hr,
):
    parts = 4
    z, y, c, me = (lax.axis_index(name) for name in ("section", "dp_0", "dp_1", "mp"))
    rows, width = patches_ref.shape
    tiles = rows // PATCH
    share = PATCH // parts
    local = width // parts
    hidden = small_ref.shape[1] // 2 - 2 * local
    block = text_ref.shape[1] // parts
    token_share = text_ref.shape[0]
    pool_share = POOL // parts

    def place_of(core, first, second):
        return first * (8 - 6 * core) + second * (2 + 6 * core) + core

    a, b = z * (1 - c) + y * c, y * (1 - c) + z * c
    pa, pb = z * c + y * (1 - c), y * c + z * (1 - c)

    def along_a(step):
        return {"section": lax.rem(z + (1 - c) * step, 4), "dp_0": lax.rem(y + c * step, 4)}

    def along_b(step):
        return {"section": lax.rem(z + c * step, 4), "dp_0": lax.rem(y + (1 - c) * step, 4)}

    def along_x(step):
        return {"mp": lax.rem(me + step, parts)}

    partner = {"dp_1": 1 - c}
    full, own_piece = (sm, pj), (small_ref, proj_ref)

    def remote(src, dst, send, recv, target):
        return pltpu.make_async_remote_copy(
            src_ref=src,
            dst_ref=dst,
            send_sem=send,
            recv_sem=recv,
            device_id=target,
            device_id_type=MESH,
        )

    def region(arr, core, first, second):
        count = own_piece[arr].shape[0]
        at = place_of(core, lax.rem(first, 4), lax.rem(second, 4))
        return full[arr].at[pl.ds(pl.multiple_of(at * count, count), count), :]

    def share_out(arr, kind, ra, rb, target):
        dst = region(arr, c, a + ra, b + rb)
        src = own_piece[arr] if (ra, rb) == (0, 0) else dst
        return remote(src, dst, gs.at[arr, kind], gr.at[arr, kind], target)

    started = ([], [])

    def give(arr, kind, ra, rb, target):
        copy = share_out(arr, kind, ra, rb, target)
        copy.start()
        started[arr].append(copy)

    def take(arr, kind, ra, rb):
        share_out(arr, kind, ra, rb, partner).wait_recv()

    def to_both(arr, ra):
        give(arr, 3 + ra, ra, 0, along_b(1))
        give(arr, 7 + ra, ra, 0, along_b(3))
        give(arr, 15 + ra * 4, ra, 0, partner)

    def gather_start(arr):
        give(arr, 0, 0, 0, along_a(1))
        give(arr, 1, 0, 0, along_a(3))
        to_both(arr, 0)
        pltpu.make_async_copy(own_piece[arr], region(arr, c, a, b), loc.at[arr]).start()

    def gather_a(arr):
        take(arr, 0, 3, 0)
        if arr == 0:
            give(arr, 2, 3, 0, along_a(1))
        to_both(arr, 3)
        take(arr, 1, 1, 0)
        if arr == 1:
            give(arr, 2, 1, 0, along_a(3))
        to_both(arr, 1)
        take(arr, 2, 2, 0)
        to_both(arr, 2)

    def gather_b(arr):
        for ra in (0, 3, 1, 2):
            take(arr, 3 + ra, ra, 3)
            if ra < 2:
                give(arr, 11 + ra, ra, 3, along_b(1))
            give(arr, 15 + ra * 4 + 3, ra, 3, partner)
            take(arr, 7 + ra, ra, 1)
            if ra >= 2:
                give(arr, 11 + ra, ra, 1, along_b(3))
            give(arr, 15 + ra * 4 + 1, ra, 1, partner)

    def gather_b2(arr):
        for ra in (0, 3, 1, 2):
            take(arr, 11 + ra, ra, 2)
            give(arr, 15 + ra * 4 + 2, ra, 2, partner)

    def gather_end(arr):
        for ra in range(4):
            for rb in range(4):
                kind = 15 + ra * 4 + rb
                dst = region(arr, 1 - c, pa + ra, pb + rb)
                remote(dst, dst, gs.at[arr, kind], gr.at[arr, kind], partner).wait_recv()
        pltpu.make_async_copy(own_piece[arr], region(arr, c, a, b), loc.at[arr]).wait()

    def count_copy(stage, step):
        name = ("mp", "dp_1", "dp_0", "section")[stage]
        at = (me, c, y, z)[stage]
        size = (4, 2, 4, 4)[stage]
        return remote(
            cbuf.at[stage, 3],
            cbuf.at[stage, step - 1],
            cs.at[stage, step - 1],
            cr.at[stage, step - 1],
            {name: lax.rem(at + step, size)},
        )

    def count_steps(stage):
        return (1,) if stage == 1 else (1, 2, 3)

    def count_send(stage):
        for step in count_steps(stage):
            count_copy(stage, step).start()

    def count_sum(stage):
        total = cbuf[stage, 3]
        for step in count_steps(stage):
            count_copy(stage, step).wait()
            total = total + cbuf[stage, step - 1]
        return total

    def text_copy(kind, incoming):
        if incoming:
            back = (3, 3, 1, 1, 2, 2)[kind]
        else:
            back = (0, 0, 0, 0, 3, 1)[kind]
        size = text_ref.shape[1] // 2
        cols = pl.ds((0, 1, 1, 0, 0, 1)[kind] * size, size)
        at = pl.multiple_of(lax.rem(me + back, parts) * token_share, token_share)
        dst = whole.at[pl.ds(at, token_share), cols]
        src = dst if incoming or kind >= 4 else text_ref.at[:, cols]
        return remote(src, dst, ts.at[kind], tr.at[kind], along_x((1, 1, 3, 3, 1, 3)[kind]))

    def text_pass():
        text_copy(0, True).wait_recv()
        text_copy(4, False).start()
        text_copy(2, True).wait_recv()
        text_copy(5, False).start()

    def text_wait():
        for kind in (1, 3, 4, 5):
            text_copy(kind, True).wait_recv()
        for kind in range(6):
            text_copy(kind, False).wait_send()

    def scatter_copy(stage, tile, step):
        target = lax.rem(me + step, parts)
        return remote(
            part.at[stage, tile, pl.ds(pl.multiple_of(target * share, share), share), :],
            rsb.at[stage, tile, step - 1],
            xs.at[2 * stage, tile, step - 1],
            xr.at[2 * stage, tile, step - 1],
            along_x(step),
        )

    def spread_copy(stage, tile, step):
        if stage == 0:
            ref = n2.at[tile, pl.ds(pl.multiple_of(me * share, share), share), :]
        else:
            ref = pooled.at[
                pl.ds(pl.multiple_of(tile * POOL + me * pool_share, pool_share), pool_share), :
            ]
        return remote(
            ref, ref, xs.at[2 * stage + 1, tile, step - 1], xr.at[2 * stage + 1, tile, step - 1], along_x(step)
        )

    def normed(wide, at):
        center = wide - jnp.mean(wide, axis=1, keepdims=True)
        spread = jnp.mean(center * center, axis=1, keepdims=True)
        scaled = center * lax.rsqrt(spread + EPS) * gain_ref[at : at + 1, :]
        return (scaled + bias_ref[at : at + 1, :]).astype(jnp.bfloat16)

    def own_sum(stage, tile):
        mine = pl.ds(pl.multiple_of(me * share, share), share)
        total = part[stage, tile, mine, :].astype(jnp.float32)
        for step in (1, 3, 2):
            scatter_copy(stage, tile, step).wait()
            total = total + rsb[stage, tile, step - 1].astype(jnp.float32)
        return total

    barrier = pltpu.get_barrier_semaphore()
    others = [{"section": lax.rem(z + step, 4)} for step in (1, 2, 3)]
    others += [{"dp_0": lax.rem(y + step, 4)} for step in (1, 2, 3)]
    others += [along_x(step) for step in (1, 2, 3)] + [partner]
    for target in others:
        pl.semaphore_signal(barrier, inc=1, device_id=target, device_id_type=MESH)
    mask = mask_ref[...].astype(jnp.float32)
    cbuf[0, 3] = jnp.broadcast_to(jnp.sum(mask, axis=1, keepdims=True), cbuf.shape[2:])
    pl.semaphore_wait(barrier, len(others))
    gather_start(0)
    gather_start(1)
    count_send(0)
    for kind in (0, 2, 1, 3):
        text_copy(kind, False).start()
    own_rows = pl.ds(pl.multiple_of(me * token_share, token_share), token_share)
    whole[own_rows, :] = text_ref[...]
    first = normed(patches_ref[...].astype(jnp.float32), 0)
    gather_a(0)
    gather_a(1)
    gather_b(0)
    gather_b2(0)
    cbuf[1, 3] = count_sum(0)
    count_send(1)
    text_pass()
    gather_end(0)
    joined[...] = jnp.dot(first, sm[:, : 3 * local], preferred_element_type=jnp.float32)
    low = lax.broadcasted_iota(jnp.int32, (PATCH, 2 * VHD), 1) < VHD

    def attend(tile):
        at = pl.ds(tile * PATCH, PATCH)
        for pair in range(local // (2 * VHD)):
            start = pair * 2 * VHD
            query = joined[at, start : start + 2 * VHD]
            keyed = joined[at, local + start : local + start + 2 * VHD].astype(jnp.bfloat16)
            valued = joined[at, 2 * local + start : 2 * local + start + 2 * VHD]
            valued = valued.astype(jnp.bfloat16)
            found = []
            for side in (low, jnp.logical_not(low)):
                masked = jnp.where(side, query, 0.0).astype(jnp.bfloat16)
                scores = lax.dot_general(
                    masked, keyed, (((1,), (1,)), ((), ())), preferred_element_type=jnp.float32
                )
                scores = scores * VHD ** (-0.5)
                probs = jnp.exp(scores - jnp.max(scores, axis=1, keepdims=True))
                total = jnp.sum(probs, axis=1, keepdims=True)
                product = jnp.dot(
                    probs.astype(jnp.bfloat16), valued, preferred_element_type=jnp.float32
                )
                found.append(product / total)
            mix[at, start : start + 2 * VHD] = jnp.where(low, *found).astype(jnp.bfloat16)
        partial_sum = lax.dot_general(
            mix[at, :],
            sm[:, 3 * local : 4 * local],
            (((1,), (1,)), ((), ())),
            preferred_element_type=jnp.float32,
        )
        part[0, tile] = partial_sum.astype(jnp.bfloat16)
        for step in (1, 3, 2):
            scatter_copy(0, tile, step).start()

    def middle(tile):
        mine = pl.ds(pl.multiple_of(tile * PATCH + me * share, share), share)
        total = patches_ref[mine, :].astype(jnp.float32) + own_sum(0, tile)
        kept = total.astype(jnp.bfloat16)
        res[tile] = kept
        rows_here = pl.ds(pl.multiple_of(me * share, share), share)
        n2[tile, rows_here, :] = normed(kept.astype(jnp.float32), 1)
        for step in (1, 3, 2):
            spread_copy(0, tile, step).start()

    def expand(tile):
        for step in (1, 3, 2):
            spread_copy(0, tile, step).wait()
        inner = jnp.dot(
            n2[tile],
            sm[:, 4 * local : 4 * local + hidden],
            preferred_element_type=jnp.float32,
        )
        inner = (0.5 * inner * (1.0 + lax.erf(inner * 0.5**0.5))).astype(jnp.bfloat16)
        partial_sum = lax.dot_general(
            inner,
            sm[:, 4 * local + hidden :],
            (((1,), (1,)), ((), ())),
            preferred_element_type=jnp.float32,
        )
        part[1, tile] = partial_sum.astype(jnp.bfloat16)
        for step in (1, 3, 2):
            scatter_copy(1, tile, step).start()

    row_at = lax.broadcasted_iota(jnp.int32, (share, share), 0)
    col_at = lax.broadcasted_iota(jnp.int32, (share, share), 1)
    quad, token = row_at // pool_share, row_at % pool_share
    side = GRID // 2
    origin = 2 * GRID * (token // side) + GRID * (quad // 2) + 2 * (token % side) + quad % 2
    shuffle = (col_at == origin).astype(jnp.float32).astype(jnp.bfloat16)

    def pool(tile):
        kept = (res[tile].astype(jnp.float32) + own_sum(1, tile)).astype(jnp.bfloat16)
        moved = jnp.dot(shuffle, kept, preferred_element_type=jnp.float32).astype(jnp.bfloat16)
        mine = pl.ds(pl.multiple_of(tile * POOL + me * pool_share, pool_share), pool_share)
        for at in range(4):
            pooled[mine, at * width : (at + 1) * width] = moved[
                at * pool_share : (at + 1) * pool_share, :
            ]
        for step in (1, 3, 2):
            spread_copy(1, tile, step).start()

    attend(0)
    gather_b(1)
    attend(1)
    middle(0)
    gather_b2(1)
    middle(1)
    cbuf[2, 3] = count_sum(1)
    count_send(2)
    text_wait()
    for tile in range(tiles):
        expand(tile)
    for tile in range(tiles):
        pool(tile)
    cbuf[3, 3] = count_sum(2)
    count_send(3)
    gather_end(1)
    for tile in range(tiles):
        for step in (1, 3, 2):
            spread_copy(1, tile, step).wait()
    image = jnp.dot(pooled[...], pj[...], preferred_element_type=jnp.float32).astype(jnp.bfloat16)
    send_row = lax.broadcasted_iota(jnp.int32, (4 * POOL, tiles * POOL), 0)
    send_col = lax.broadcasted_iota(jnp.int32, (4 * POOL, tiles * POOL), 1)
    chosen = (own_ref[...] == send_row // POOL) & (send_row % POOL == send_col % POOL)
    chosen = chosen.astype(jnp.float32).astype(jnp.bfloat16)
    blk[...] = jnp.dot(chosen, image, preferred_element_type=jnp.float32).astype(jnp.bfloat16)

    def home_copy(step):
        target = lax.rem(z + step, 4)
        return remote(
            blk.at[pl.ds(pl.multiple_of(target * POOL, POOL), POOL), :],
            arrived.at[pl.ds(pl.multiple_of(z * POOL, POOL), POOL), :],
            zs.at[step - 1],
            zr.at[step - 1],
            {"section": target},
        )

    for step in (2, 1, 3):
        home_copy(step).start()
    here = pl.ds(pl.multiple_of(z * POOL, POOL), POOL)
    arrived[here, :] = blk[here, :]
    count = count_sum(3)
    scaling = float(4 * 8 * parts * token_share)
    weight_ref[...] = mask * scaling / count[:1, :]
    length = state_ref.shape[0]
    picked = lax.broadcasted_iota(jnp.int32, (length, 4 * POOL), 0) == place_ref[...]
    picked = picked.astype(jnp.float32)
    covered = jnp.max(picked, axis=1, keepdims=True) > 0.5
    for copies_of in started:
        for copy in copies_of:
            copy.wait_send()
    for step in (1, 3, 2):
        home_copy(step).wait()
    half = block // 2

    def state_copy(kind, incoming):
        if incoming:
            back = (3, 3, 1, 1, 2, 2)[kind]
        else:
            back = (0, 0, 0, 0, 3, 1)[kind]
        at = lax.rem(me + back, parts) * block + (0, 1, 1, 0, 0, 1)[kind] * half
        ref = images.at[:, pl.ds(pl.multiple_of(at, half), half)]
        return remote(ref, ref, hs.at[kind], hr.at[kind], along_x((1, 1, 3, 3, 1, 3)[kind]))

    images[:, pl.ds(pl.multiple_of(me * block, block), block)] = arrived[...]
    for kind in (0, 2, 1, 3):
        state_copy(kind, False).start()
    state_copy(0, True).wait_recv()
    state_copy(4, False).start()
    state_copy(2, True).wait_recv()
    state_copy(5, False).start()
    picked = picked.astype(jnp.bfloat16)

    def settle(back):
        cols = pl.ds(pl.multiple_of(lax.rem(me + back, parts) * block, block), block)
        placed = jnp.dot(picked, images[:, cols], preferred_element_type=jnp.float32)
        kept = jnp.where(covered, placed, whole[:, cols].astype(jnp.float32))
        state_ref[:, cols] = kept.astype(jnp.bfloat16)

    settle(0)
    state_copy(1, True).wait_recv()
    settle(3)
    state_copy(3, True).wait_recv()
    settle(1)
    for kind in (4, 5):
        state_copy(kind, True).wait_recv()
    settle(2)
    for kind in range(6):
        state_copy(kind, False).wait_send()


def encode(patches, vis_gain, vis_bias, text, mask, own, place, small, proj):
    rows, width = patches.shape
    tiles = rows // PATCH
    block = text.shape[1] // 4
    length = text.shape[0] * 4
    share = PATCH // 4
    dma = pltpu.SemaphoreType.DMA
    vmem = pl.BlockSpec(memory_space=pltpu.VMEM)
    bf16 = jnp.bfloat16
    return pl.pallas_call(
        vision_kernel,
        out_shape=(
            jax.ShapeDtypeStruct((length, 4 * block), bf16),
            jax.ShapeDtypeStruct(mask.shape, jnp.float32),
        ),
        in_specs=[vmem] * 9,
        out_specs=(vmem, vmem),
        scratch_shapes=[
            pltpu.VMEM((small.shape[0] * 32, small.shape[1]), bf16),
            pltpu.VMEM((proj.shape[0] * 32, proj.shape[1]), bf16),
            pltpu.VMEM((rows, 3 * width // 4), jnp.float32),
            pltpu.VMEM((rows, width // 4), bf16),
            pltpu.VMEM((2, tiles, PATCH, width), bf16),
            pltpu.VMEM((2, tiles, 3, share, width), bf16),
            pltpu.VMEM((tiles, share, width), bf16),
            pltpu.VMEM((tiles, PATCH, width), bf16),
            pltpu.VMEM((tiles * POOL, 4 * width), bf16),
            pltpu.VMEM((4 * POOL, block), bf16),
            pltpu.VMEM((4 * POOL, block), bf16),
            pltpu.VMEM((4 * POOL, 4 * block), bf16),
            pltpu.VMEM((4, 4, 8, 128), jnp.float32),
            dma((2, 31)),
            dma((2, 31)),
            dma((4, tiles, 3)),
            dma((4, tiles, 3)),
            dma((3,)),
            dma((3,)),
            dma((6,)),
            dma((6,)),
            dma((4, 3)),
            dma((4, 3)),
            dma((2,)),
            pltpu.VMEM((length, 4 * block), bf16),
            dma((6,)),
            dma((6,)),
        ],
        compiler_params=pltpu.CompilerParams(
            collective_id=1, has_side_effects=True, vmem_limit_bytes=56 * 1024 * 1024
        ),
    )(patches, vis_gain, vis_bias, text, mask, own, place, small, proj)


def decoder_kernel(
    seg_col,
    seg_row,
    cos_ref,
    sin_ref,
    s0_ref,
    w_any,
    out_ref,
    xbuf,
    mbuf,
    wjb,
    wob,
    acc,
    ssq,
    kb,
    vb,
    bias,
    fin,
    hid,
    xs,
    xr,
    ms,
    mr,
    js,
    os,
    fs,
    fr,
    rs,
):
    parts = 4
    layers = 4
    copies = w_any.shape[0] // layers
    length = s0_ref.shape[0]
    block = s0_ref.shape[1] // parts
    half = length // 2
    joined = wjb.shape[2]
    query_width = wob.shape[1] // parts
    heads = query_width // HD
    depth = w_any.shape[1]
    col_share = wob.shape[2] // copies
    token_share = length // parts
    me = lax.axis_index("mp")
    right, opposite, left = (lax.rem(me + step, parts) for step in (1, 2, 3))

    def weight_copies(layer, par):
        found = []
        for d in range(copies):
            found.append(
                pltpu.make_async_copy(
                    w_any.at[layer * copies + d, :, pl.ds(0, joined)],
                    wjb.at[par, pl.ds(d * depth, depth), :],
                    js.at[par, d],
                )
            )
        for d in range(copies):
            for part in range(parts):
                found.append(
                    pltpu.make_async_copy(
                        w_any.at[
                            layer * copies + d, :, pl.ds(joined + part * col_share, col_share)
                        ],
                        wob.at[par, pl.ds(part * depth, depth), pl.ds(d * col_share, col_share)],
                        os.at[par, d * parts + part],
                    )
                )
        return found[:copies], found[copies:]

    def piece(buf, width, sends, recvs, par, h, kind, source, half_at, target):
        cols = pl.ds(pl.multiple_of(source * width + half_at * (width // 2), width // 2), width // 2)
        ref = buf.at[par, pl.ds(h * half, half), cols]
        return pltpu.make_async_remote_copy(
            src_ref=ref,
            dst_ref=ref,
            send_sem=sends.at[par, h, kind],
            recv_sem=recvs.at[par, h, kind],
            device_id={"mp": target},
            device_id_type=MESH,
        )

    def sent(kind, buf, width, sends, recvs, par, h):
        source, half_at, target = (
            (me, 0, right),
            (me, 1, right),
            (me, 1, left),
            (me, 0, left),
            (left, 0, right),
            (right, 1, left),
        )[kind]
        return piece(buf, width, sends, recvs, par, h, kind, source, half_at, target)

    def landed(kind, buf, width, sends, recvs, par, h):
        source, half_at = (
            (left, 0),
            (left, 1),
            (right, 1),
            (right, 0),
            (opposite, 0),
            (opposite, 1),
        )[kind]
        return piece(buf, width, sends, recvs, par, h, kind, source, half_at, right)

    x_args = (xbuf, block, xs, xr)
    m_args = (mbuf, query_width, ms, mr)

    def forward(args, par, h):
        landed(0, *args, par, h).wait_recv()
        sent(4, *args, par, h).start()
        landed(2, *args, par, h).wait_recv()
        sent(5, *args, par, h).start()

    def waits(args, par, h, kinds):
        for kind in kinds:
            landed(kind, *args, par, h).wait_recv()

    def wait_sends(args, par, h):
        for kind in range(6):
            sent(kind, *args, par, h).wait_send()

    def start_own(par, h):
        for kind in (0, 2, 1, 3):
            sent(kind, *x_args, par, h).start()

    first_joined, first_out = weight_copies(0, 0)
    for copy in first_joined + first_out:
        copy.start()
    barrier = pltpu.get_barrier_semaphore()
    for target in (right, opposite, left):
        pl.semaphore_signal(barrier, inc=1, device_id={"mp": target}, device_id_type=MESH)
    own_cols = pl.ds(pl.multiple_of(me * block, block), block)
    ready = pltpu.make_async_copy(s0_ref, xbuf.at[0], rs.at[0])
    ready.start()
    rows_at = lax.broadcasted_iota(jnp.int32, (length, length), 0)
    cols_at = lax.broadcasted_iota(jnp.int32, (length, length), 1)
    allowed = (seg_col[...] == seg_row[...]) & (cols_at <= rows_at)
    bias[...] = jnp.where(allowed, 0.0, BLOCKED)
    pl.semaphore_wait(barrier, 3)
    ready.wait()

    def project(par, h, layer):
        rows = pl.ds(h * half, half)

        def add(source, first):
            cols = pl.ds(pl.multiple_of(source * block, block), block)
            values = xbuf[par, rows, cols]
            product = jnp.dot(values, wjb[par, cols, :], preferred_element_type=jnp.float32)
            wide = values.astype(jnp.float32)
            wide = wide * wide
            power = wide[:, :HD]
            for at in range(1, block // HD):
                power = power + wide[:, at * HD : (at + 1) * HD]
            if first:
                acc[:, :joined] = product
                ssq[...] = power
            else:
                acc[:, :joined] += product
                ssq[...] += power

        def arrive(step):
            @pl.when(layer > 0)
            def _():
                step()

        add(me, True)
        if h == 1:
            arrive(lambda: forward(x_args, par, h))
        arrive(lambda: waits(x_args, par, h, (1,)))
        add(left, False)
        arrive(lambda: waits(x_args, par, h, (3,)))
        add(right, False)
        if h == 1:
            forward(m_args, par, 0)
        arrive(lambda: waits(x_args, par, h, (4, 5)))
        add(opposite, False)

    def attend(par, h):
        rows = pl.ds(h * half, half)
        keys = half * (h + 1)
        power = jnp.sum(ssq[...], axis=1, keepdims=True) * (1.0 / (parts * block))
        scale = lax.rsqrt(power + EPS)
        cosine = cos_ref[rows, :] * scale
        sinus = sin_ref[rows, :] * scale

        def turned(at):
            values = acc[:, at * HD : (at + 1) * HD]
            return values * cosine + pltpu.roll(values, HD // 2, 1) * sinus

        kb[rows, :] = turned(heads).astype(jnp.bfloat16)
        vb[rows, :] = (acc[:, (heads + 1) * HD : (heads + 2) * HD] * scale).astype(jnp.bfloat16)
        for head in range(heads):
            query = (turned(head) * HD ** (-0.5)).astype(jnp.bfloat16)
            scores = lax.dot_general(
                query,
                kb[:keys, :],
                (((1,), (1,)), ((), ())),
                preferred_element_type=jnp.float32,
            )
            scores = scores + bias[rows, :keys]
            top = jnp.max(scores, axis=1, keepdims=True)
            probs = jnp.exp(scores - top)
            total = jnp.sum(probs, axis=1, keepdims=True)
            mixed = jnp.dot(
                probs.astype(jnp.bfloat16), vb[:keys, :], preferred_element_type=jnp.float32
            )
            cols = pl.ds(pl.multiple_of(me * query_width + head * HD, HD), HD)
            mbuf[par, rows, cols] = (mixed / total).astype(jnp.bfloat16)
            if head == heads // 2 - 1:
                sent(0, *m_args, par, h).start()
                sent(3, *m_args, par, h).start()
        sent(2, *m_args, par, h).start()
        sent(1, *m_args, par, h).start()

    def shared(target, source):
        return pltpu.make_async_remote_copy(
            src_ref=fin.at[pl.ds(target * token_share, token_share), :],
            dst_ref=hid.at[:, pl.ds(pl.multiple_of(source * block, block), block)],
            send_sem=fs.at[target],
            recv_sem=fr.at[source],
            device_id={"mp": target},
            device_id_type=MESH,
        )

    def leave(par, h, layer):
        rows = pl.ds(h * half, half)

        def term(source):
            cols = pl.ds(pl.multiple_of(source * query_width, query_width), query_width)
            return jnp.dot(
                mbuf[par, rows, cols], wob[par, cols, :], preferred_element_type=jnp.float32
            )

        acc[...] = xbuf[par, rows, own_cols].astype(jnp.float32) + term(me)
        waits(m_args, par, h, (1,))
        acc[...] += term(left)
        waits(m_args, par, h, (3,))
        acc[...] += term(right)
        waits(m_args, par, h, (4, 5))

        @pl.when(layer > 0)
        def _():
            wait_sends(x_args, par, h)

        result = (acc[...] + term(opposite)).astype(jnp.bfloat16)
        if h == 0:
            forward(m_args, par, 1)

        @pl.when(layer < layers - 1)
        def _():
            xbuf[1 - par, rows, own_cols] = result
            if h == 1:
                forward(x_args, 1 - par, 0)
            start_own(1 - par, h)

        @pl.when(layer == layers - 1)
        def _():
            fin[rows, :] = result
            for target in (2 * h, 2 * h + 1):

                @pl.when(target != me)
                def _():
                    shared(target, me).start()

                @pl.when(target == me)
                def _():
                    hid[:, own_cols] = fin[target * token_share : (target + 1) * token_share, :]

    def one_layer(layer, carry):
        par = lax.rem(layer, 2)
        joined_copies, out_copies = weight_copies(layer, par)
        for copy in joined_copies:
            copy.wait()

        @pl.when(layer < layers - 1)
        def _():
            for copies_of in weight_copies(layer + 1, 1 - par):
                for copy in copies_of:
                    copy.start()

        for h in range(2):
            project(par, h, layer)

            @pl.when(layer > 0)
            def _():
                wait_sends(m_args, 1 - par, h)

            attend(par, h)
        for copy in out_copies:
            copy.wait()
        for h in range(2):
            leave(par, h, layer)
        return carry

    lax.fori_loop(0, layers, one_layer, 0)
    last = (layers - 1) % 2

    for h in range(2):
        wait_sends(m_args, last, h)
    for target in range(parts):

        @pl.when(target != me)
        def _():
            shared(target, me).wait_send()
            shared(target, target).wait_recv()

    out_ref[...] = hid[...]


def decode(state, segment_ids, weights):
    parts = lax.axis_size("mp")
    length, block = state.shape[0], state.shape[1] // parts
    copies = lax.axis_size(DP)
    depth = weights.shape[1]
    joined = weights.shape[2] - parts * (block // copies)
    cosine, sinus = rope_tables(length)
    dma = pltpu.SemaphoreType.DMA
    vmem = pl.BlockSpec(memory_space=pltpu.VMEM)
    return pl.pallas_call(
        decoder_kernel,
        out_shape=jax.ShapeDtypeStruct((length // parts, parts * block), jnp.bfloat16),
        in_specs=[vmem] * 4 + [pl.BlockSpec(memory_space=pl.ANY)] * 2,
        out_specs=vmem,
        scratch_shapes=[
            pltpu.VMEM((2, length, parts * block), jnp.bfloat16),
            pltpu.VMEM((2, length, parts * depth), jnp.bfloat16),
            pltpu.VMEM((2, copies * depth, joined), jnp.bfloat16),
            pltpu.VMEM((2, parts * depth, block), jnp.bfloat16),
            pltpu.VMEM((length // 2, block), jnp.float32),
            pltpu.VMEM((length // 2, HD), jnp.float32),
            pltpu.VMEM((length, HD), jnp.bfloat16),
            pltpu.VMEM((length, HD), jnp.bfloat16),
            pltpu.VMEM((length, length), jnp.float32),
            pltpu.VMEM((length, block), jnp.bfloat16),
            pltpu.VMEM((length // parts, parts * block), jnp.bfloat16),
            dma((2, 2, 6)),
            dma((2, 2, 6)),
            dma((2, 2, 6)),
            dma((2, 2, 6)),
            dma((2, copies)),
            dma((2, copies * parts)),
            dma((4,)),
            dma((4,)),
            dma((1,)),
        ],
        compiler_params=pltpu.CompilerParams(
            collective_id=0, has_side_effects=True, vmem_limit_bytes=60 * 1024 * 1024
        ),
    )(segment_ids[:, None], segment_ids[None, :], cosine, sinus, state, weights)


def shards(
    text,
    patches,
    segments,
    loss_mask,
    tile_batch,
    tile_offset,
    attn_gain,
    w_query,
    w_kv,
    w_out,
    vis_gain,
    vis_bias,
    v_qkv,
    v_out,
    v_up,
    v_down,
    v_proj,
):
    section_at = lax.axis_index("section")
    parts = lax.axis_size("mp")
    copies = lax.axis_size(DP)
    copy_at = lax.axis_index(DP)
    model_width = w_query.shape[1]
    row_share = model_width // copies
    pick = lambda array: lax.dynamic_slice_in_dim(array, copy_at * row_share, row_share, 0)
    own_rows = jnp.concatenate([pick(w_query[0]), pick(w_kv[0, 0]), pick(w_kv[0, 1])], axis=1)
    own_gain = lax.dynamic_slice_in_dim(attn_gain[0], copy_at * row_share, row_share, 0)
    own_rows = (own_rows.astype(jnp.float32) * own_gain[:, None]).astype(jnp.bfloat16)
    block_width = model_width // parts
    col_share = block_width // copies
    own_out = [
        lax.dynamic_slice_in_dim(w_out[0], part * block_width + copy_at * col_share, col_share, 1)
        for part in range(parts)
    ]
    own_out = lax.all_to_all(
        jnp.stack(own_out), "mp", split_axis=0, concat_axis=0, tiled=True
    )
    own_out = jnp.concatenate([own_out[part] for part in range(parts)], axis=1)
    own = jnp.concatenate([own_rows, own_out], axis=1)
    own, v_out, v_down = lax.optimization_barrier((own, v_out, v_down))
    small = jnp.concatenate([v_qkv[0], v_qkv[1], v_qkv[2], v_out.T, v_up, v_down.T], axis=1)
    sections = lax.axis_size("section")
    batch_all = tile_batch[0].reshape(sections, -1)
    offset_all = tile_offset[0].reshape(sections, -1)
    own_batch = lax.dynamic_slice_in_dim(batch_all, section_at, 1, 0)
    own_batch = jnp.repeat(own_batch, POOL, axis=1)
    starts = jnp.max(jnp.where(batch_all == section_at, offset_all, -POOL), axis=1)
    place = jnp.repeat(starts, POOL) + jnp.tile(jnp.arange(POOL, dtype=jnp.int32), sections)
    weights = lax.all_gather(own, SECTION_DP)
    state, token_weight = encode(
        patches,
        vis_gain,
        vis_bias,
        text[0],
        loss_mask,
        own_batch,
        place[None, :],
        small,
        v_proj,
    )
    hidden = decode(state, segments[0, 0], weights)
    return (hidden[None], token_weight)


def solution(mesh):
    split = Mesh(
        mesh.devices.reshape(mesh.shape["section"], 4, 2, mesh.shape["mp"]),
        ("section", "dp_0", "dp_1", "mp"),
    )
    return jax.shard_map(
        shards,
        mesh=split,
        in_specs=(
            P("section", DP_MP, None),
            P(SECTION_DP, None),
            P("section", DP, None),
            P("section", DP_MP),
            P(DP, None),
            P(DP, None),
            P("section", None),
            P("section", None, "mp"),
            P("section", None, None, "mp"),
            P("section", "mp", None),
            P(),
            P(),
            P(None, SECTION_DP, "mp"),
            P("mp", SECTION_DP),
            P(SECTION_DP, "mp"),
            P("mp", SECTION_DP),
            P(SECTION_DP, "mp"),
        ),
        out_specs=(P("section", DP_MP, None), P("section", DP_MP)),
        check_vma=False,
    )
```

```python
import jax
import jax.numpy as jnp
from jax import lax
from jax.experimental import pallas as pl
from jax.experimental.pallas import tpu as pltpu
from jax.sharding import Mesh
from jax.sharding import PartitionSpec as P

HD = 128
VHD = 64
GRID = 16
PATCH = 256
POOL = 64
SECTION_DP = ("section", "dp_0", "dp_1")
SECTION_DP_MP = ("section", "dp_0", "dp_1", "mp")
DP = ("dp_0", "dp_1")
DP_MP = ("dp_0", "dp_1", "mp")


EPS = 1e-05
ROPE_BASE = 500000.0
BLOCKED = -1e30
MESH = pl.DeviceIdType.MESH


def rope_tables(length):
    half_width = HD // 2
    freqs = ROPE_BASE ** (-2.0 * jnp.arange(half_width, dtype=jnp.float32) / HD)
    angles = jnp.arange(length, dtype=jnp.float32)[:, None] * freqs[None, :]
    cosine, sinus = jnp.cos(angles), jnp.sin(angles)
    return (
        jnp.concatenate([cosine, cosine], axis=1),
        jnp.concatenate([-sinus, sinus], axis=1),
    )


def vision_kernel(
    patches_ref,
    gain_ref,
    bias_ref,
    text_ref,
    mask_ref,
    own_ref,
    place_ref,
    small_ref,
    proj_ref,
    state_ref,
    weight_ref,
    sm,
    pj,
    joined,
    mix,
    part,
    rsb,
    res,
    n2,
    pooled,
    blk,
    arrived,
    images,
    cbuf,
    gs,
    gr,
    xs,
    xr,
    zs,
    zr,
    ts,
    tr,
    cs,
    cr,
    loc,
    whole,
    hs,
    hr,
):
    parts = 4
    z, y, c, me = (lax.axis_index(name) for name in ("section", "dp_0", "dp_1", "mp"))
    rows, width = patches_ref.shape
    tiles = rows // PATCH
    share = PATCH // parts
    local = width // parts
    hidden = small_ref.shape[1] // 2 - 2 * local
    block = text_ref.shape[1] // parts
    token_share = text_ref.shape[0]
    pool_share = POOL // parts

    def place_of(core, first, second):
        return first * (8 - 6 * core) + second * (2 + 6 * core) + core

    a, b = z * (1 - c) + y * c, y * (1 - c) + z * c
    pa, pb = z * c + y * (1 - c), y * c + z * (1 - c)

    def along_a(step):
        return {"section": lax.rem(z + (1 - c) * step, 4), "dp_0": lax.rem(y + c * step, 4)}

    def along_b(step):
        return {"section": lax.rem(z + c * step, 4), "dp_0": lax.rem(y + (1 - c) * step, 4)}

    def along_x(step):
        return {"mp": lax.rem(me + step, parts)}

    partner = {"dp_1": 1 - c}
    full, own_piece = (sm, pj), (small_ref, proj_ref)

    def remote(src, dst, send, recv, target):
        return pltpu.make_async_remote_copy(
            src_ref=src,
            dst_ref=dst,
            send_sem=send,
            recv_sem=recv,
            device_id=target,
            device_id_type=MESH,
        )

    def region(arr, core, first, second):
        count = own_piece[arr].shape[0]
        at = place_of(core, lax.rem(first, 4), lax.rem(second, 4))
        return full[arr].at[pl.ds(pl.multiple_of(at * count, count), count), :]

    def share_out(arr, kind, ra, rb, target):
        dst = region(arr, c, a + ra, b + rb)
        src = own_piece[arr] if (ra, rb) == (0, 0) else dst
        return remote(src, dst, gs.at[arr, kind], gr.at[arr, kind], target)

    started = ([], [])

    def give(arr, kind, ra, rb, target):
        copy = share_out(arr, kind, ra, rb, target)
        copy.start()
        started[arr].append(copy)

    def take(arr, kind, ra, rb):
        share_out(arr, kind, ra, rb, partner).wait_recv()

    def to_both(arr, ra):
        give(arr, 3 + ra, ra, 0, along_b(1))
        give(arr, 7 + ra, ra, 0, along_b(3))
        give(arr, 15 + ra * 4, ra, 0, partner)

    def gather_start(arr):
        give(arr, 0, 0, 0, along_a(1))
        give(arr, 1, 0, 0, along_a(3))
        to_both(arr, 0)
        pltpu.make_async_copy(own_piece[arr], region(arr, c, a, b), loc.at[arr]).start()

    def gather_a(arr):
        take(arr, 0, 3, 0)
        if arr == 0:
            give(arr, 2, 3, 0, along_a(1))
        to_both(arr, 3)
        take(arr, 1, 1, 0)
        if arr == 1:
            give(arr, 2, 1, 0, along_a(3))
        to_both(arr, 1)
        take(arr, 2, 2, 0)
        to_both(arr, 2)

    def gather_b(arr):
        for ra in (0, 3, 1, 2):
            take(arr, 3 + ra, ra, 3)
            if ra < 2:
                give(arr, 11 + ra, ra, 3, along_b(1))
            give(arr, 15 + ra * 4 + 3, ra, 3, partner)
            take(arr, 7 + ra, ra, 1)
            if ra >= 2:
                give(arr, 11 + ra, ra, 1, along_b(3))
            give(arr, 15 + ra * 4 + 1, ra, 1, partner)

    def gather_b2(arr):
        for ra in (0, 3, 1, 2):
            take(arr, 11 + ra, ra, 2)
            give(arr, 15 + ra * 4 + 2, ra, 2, partner)

    def gather_end(arr):
        for ra in range(4):
            for rb in range(4):
                kind = 15 + ra * 4 + rb
                dst = region(arr, 1 - c, pa + ra, pb + rb)
                remote(dst, dst, gs.at[arr, kind], gr.at[arr, kind], partner).wait_recv()
        pltpu.make_async_copy(own_piece[arr], region(arr, c, a, b), loc.at[arr]).wait()

    def count_copy(stage, step):
        name = ("mp", "dp_1", "dp_0", "section")[stage]
        at = (me, c, y, z)[stage]
        size = (4, 2, 4, 4)[stage]
        return remote(
            cbuf.at[stage, 3],
            cbuf.at[stage, step - 1],
            cs.at[stage, step - 1],
            cr.at[stage, step - 1],
            {name: lax.rem(at + step, size)},
        )

    def count_steps(stage):
        return (1,) if stage == 1 else (1, 2, 3)

    def count_send(stage):
        for step in count_steps(stage):
            count_copy(stage, step).start()

    def count_sum(stage):
        total = cbuf[stage, 3]
        for step in count_steps(stage):
            count_copy(stage, step).wait()
            total = total + cbuf[stage, step - 1]
        return total

    def text_copy(kind, incoming):
        if incoming:
            back = (3, 3, 1, 1, 2, 2)[kind]
        else:
            back = (0, 0, 0, 0, 3, 1)[kind]
        size = text_ref.shape[1] // 2
        cols = pl.ds((0, 1, 1, 0, 0, 1)[kind] * size, size)
        at = pl.multiple_of(lax.rem(me + back, parts) * token_share, token_share)
        dst = whole.at[pl.ds(at, token_share), cols]
        src = dst if incoming or kind >= 4 else text_ref.at[:, cols]
        return remote(src, dst, ts.at[kind], tr.at[kind], along_x((1, 1, 3, 3, 1, 3)[kind]))

    def text_pass():
        text_copy(0, True).wait_recv()
        text_copy(4, False).start()
        text_copy(2, True).wait_recv()
        text_copy(5, False).start()

    def text_wait():
        for kind in (1, 3, 4, 5):
            text_copy(kind, True).wait_recv()
        for kind in range(6):
            text_copy(kind, False).wait_send()

    def scatter_copy(stage, tile, step):
        target = lax.rem(me + step, parts)
        return remote(
            part.at[stage, tile, pl.ds(pl.multiple_of(target * share, share), share), :],
            rsb.at[stage, tile, step - 1],
            xs.at[2 * stage, tile, step - 1],
            xr.at[2 * stage, tile, step - 1],
            along_x(step),
        )

    def spread_copy(stage, tile, step):
        if stage == 0:
            ref = n2.at[tile, pl.ds(pl.multiple_of(me * share, share), share), :]
        else:
            ref = pooled.at[
                pl.ds(pl.multiple_of(tile * POOL + me * pool_share, pool_share), pool_share), :
            ]
        return remote(
            ref, ref, xs.at[2 * stage + 1, tile, step - 1], xr.at[2 * stage + 1, tile, step - 1], along_x(step)
        )

    def normed(wide, at):
        center = wide - jnp.mean(wide, axis=1, keepdims=True)
        spread = jnp.mean(center * center, axis=1, keepdims=True)
        scaled = center * lax.rsqrt(spread + EPS) * gain_ref[at : at + 1, :]
        return (scaled + bias_ref[at : at + 1, :]).astype(jnp.bfloat16)

    def own_sum(stage, tile):
        mine = pl.ds(pl.multiple_of(me * share, share), share)
        total = part[stage, tile, mine, :].astype(jnp.float32)
        for step in (1, 3, 2):
            scatter_copy(stage, tile, step).wait()
            total = total + rsb[stage, tile, step - 1].astype(jnp.float32)
        return total

    barrier = pltpu.get_barrier_semaphore()
    others = [{"section": lax.rem(z + step, 4)} for step in (1, 2, 3)]
    others += [{"dp_0": lax.rem(y + step, 4)} for step in (1, 2, 3)]
    others += [along_x(step) for step in (1, 2, 3)] + [partner]
    for target in others:
        pl.semaphore_signal(barrier, inc=1, device_id=target, device_id_type=MESH)
    mask = mask_ref[...].astype(jnp.float32)
    cbuf[0, 3] = jnp.broadcast_to(jnp.sum(mask, axis=1, keepdims=True), cbuf.shape[2:])
    pl.semaphore_wait(barrier, len(others))
    gather_start(0)
    gather_start(1)
    count_send(0)
    for kind in (0, 2, 1, 3):
        text_copy(kind, False).start()
    own_rows = pl.ds(pl.multiple_of(me * token_share, token_share), token_share)
    whole[own_rows, :] = text_ref[...]
    first = normed(patches_ref[...].astype(jnp.float32), 0)
    gather_a(0)
    gather_a(1)
    gather_b(0)
    gather_b2(0)
    cbuf[1, 3] = count_sum(0)
    count_send(1)
    text_pass()
    gather_end(0)
    joined[...] = jnp.dot(first, sm[:, : 3 * local], preferred_element_type=jnp.float32)
    low = lax.broadcasted_iota(jnp.int32, (PATCH, 2 * VHD), 1) < VHD

    def attend(tile):
        at = pl.ds(tile * PATCH, PATCH)
        for pair in range(local // (2 * VHD)):
            start = pair * 2 * VHD
            query = joined[at, start : start + 2 * VHD]
            keyed = joined[at, local + start : local + start + 2 * VHD].astype(jnp.bfloat16)
            valued = joined[at, 2 * local + start : 2 * local + start + 2 * VHD]
            valued = valued.astype(jnp.bfloat16)
            found = []
            for side in (low, jnp.logical_not(low)):
                masked = jnp.where(side, query, 0.0).astype(jnp.bfloat16)
                scores = lax.dot_general(
                    masked, keyed, (((1,), (1,)), ((), ())), preferred_element_type=jnp.float32
                )
                scores = scores * VHD ** (-0.5)
                probs = jnp.exp(scores - jnp.max(scores, axis=1, keepdims=True))
                total = jnp.sum(probs, axis=1, keepdims=True)
                product = jnp.dot(
                    probs.astype(jnp.bfloat16), valued, preferred_element_type=jnp.float32
                )
                found.append(product / total)
            mix[at, start : start + 2 * VHD] = jnp.where(low, *found).astype(jnp.bfloat16)
        partial_sum = lax.dot_general(
            mix[at, :],
            sm[:, 3 * local : 4 * local],
            (((1,), (1,)), ((), ())),
            preferred_element_type=jnp.float32,
        )
        part[0, tile] = partial_sum.astype(jnp.bfloat16)
        for step in (1, 3, 2):
            scatter_copy(0, tile, step).start()

    def middle(tile):
        mine = pl.ds(pl.multiple_of(tile * PATCH + me * share, share), share)
        total = patches_ref[mine, :].astype(jnp.float32) + own_sum(0, tile)
        kept = total.astype(jnp.bfloat16)
        res[tile] = kept
        rows_here = pl.ds(pl.multiple_of(me * share, share), share)
        n2[tile, rows_here, :] = normed(kept.astype(jnp.float32), 1)
        for step in (1, 3, 2):
            spread_copy(0, tile, step).start()

    def expand(tile):
        for step in (1, 3, 2):
            spread_copy(0, tile, step).wait()
        inner = jnp.dot(
            n2[tile],
            sm[:, 4 * local : 4 * local + hidden],
            preferred_element_type=jnp.float32,
        )
        inner = (0.5 * inner * (1.0 + lax.erf(inner * 0.5**0.5))).astype(jnp.bfloat16)
        partial_sum = lax.dot_general(
            inner,
            sm[:, 4 * local + hidden :],
            (((1,), (1,)), ((), ())),
            preferred_element_type=jnp.float32,
        )
        part[1, tile] = partial_sum.astype(jnp.bfloat16)
        for step in (1, 3, 2):
            scatter_copy(1, tile, step).start()

    row_at = lax.broadcasted_iota(jnp.int32, (share, share), 0)
    col_at = lax.broadcasted_iota(jnp.int32, (share, share), 1)
    quad, token = row_at // pool_share, row_at % pool_share
    side = GRID // 2
    origin = 2 * GRID * (token // side) + GRID * (quad // 2) + 2 * (token % side) + quad % 2
    shuffle = (col_at == origin).astype(jnp.float32).astype(jnp.bfloat16)

    def pool(tile):
        kept = (res[tile].astype(jnp.float32) + own_sum(1, tile)).astype(jnp.bfloat16)
        moved = jnp.dot(shuffle, kept, preferred_element_type=jnp.float32).astype(jnp.bfloat16)
        mine = pl.ds(pl.multiple_of(tile * POOL + me * pool_share, pool_share), pool_share)
        for at in range(4):
            pooled[mine, at * width : (at + 1) * width] = moved[
                at * pool_share : (at + 1) * pool_share, :
            ]
        for step in (1, 3, 2):
            spread_copy(1, tile, step).start()

    attend(0)
    gather_b(1)
    attend(1)
    middle(0)
    gather_b2(1)
    middle(1)
    cbuf[2, 3] = count_sum(1)
    count_send(2)
    text_wait()
    for tile in range(tiles):
        expand(tile)
    for tile in range(tiles):
        pool(tile)
    cbuf[3, 3] = count_sum(2)
    count_send(3)
    gather_end(1)
    for tile in range(tiles):
        for step in (1, 3, 2):
            spread_copy(1, tile, step).wait()
    image = jnp.dot(pooled[...], pj[...], preferred_element_type=jnp.float32).astype(jnp.bfloat16)
    send_row = lax.broadcasted_iota(jnp.int32, (4 * POOL, tiles * POOL), 0)
    send_col = lax.broadcasted_iota(jnp.int32, (4 * POOL, tiles * POOL), 1)
    chosen = (own_ref[...] == send_row // POOL) & (send_row % POOL == send_col % POOL)
    chosen = chosen.astype(jnp.float32).astype(jnp.bfloat16)
    blk[...] = jnp.dot(chosen, image, preferred_element_type=jnp.float32).astype(jnp.bfloat16)

    def home_copy(step):
        target = lax.rem(z + step, 4)
        return remote(
            blk.at[pl.ds(pl.multiple_of(target * POOL, POOL), POOL), :],
            arrived.at[pl.ds(pl.multiple_of(z * POOL, POOL), POOL), :],
            zs.at[step - 1],
            zr.at[step - 1],
            {"section": target},
        )

    for step in (2, 1, 3):
        home_copy(step).start()
    here = pl.ds(pl.multiple_of(z * POOL, POOL), POOL)
    arrived[here, :] = blk[here, :]
    count = count_sum(3)
    scaling = float(4 * 8 * parts * token_share)
    weight_ref[...] = mask * scaling / count[:1, :]
    length = state_ref.shape[0]
    picked = lax.broadcasted_iota(jnp.int32, (length, 4 * POOL), 0) == place_ref[...]
    picked = picked.astype(jnp.float32)
    covered = jnp.max(picked, axis=1, keepdims=True) > 0.5
    for copies_of in started:
        for copy in copies_of:
            copy.wait_send()
    for step in (1, 3, 2):
        home_copy(step).wait()
    half = block // 2

    def state_copy(kind, incoming):
        if incoming:
            back = (3, 3, 1, 1, 2, 2)[kind]
        else:
            back = (0, 0, 0, 0, 3, 1)[kind]
        at = lax.rem(me + back, parts) * block + (0, 1, 1, 0, 0, 1)[kind] * half
        ref = images.at[:, pl.ds(pl.multiple_of(at, half), half)]
        return remote(ref, ref, hs.at[kind], hr.at[kind], along_x((1, 1, 3, 3, 1, 3)[kind]))

    images[:, pl.ds(pl.multiple_of(me * block, block), block)] = arrived[...]
    for kind in (0, 2, 1, 3):
        state_copy(kind, False).start()
    state_copy(0, True).wait_recv()
    state_copy(4, False).start()
    state_copy(2, True).wait_recv()
    state_copy(5, False).start()
    picked = picked.astype(jnp.bfloat16)

    def settle(back):
        cols = pl.ds(pl.multiple_of(lax.rem(me + back, parts) * block, block), block)
        placed = jnp.dot(picked, images[:, cols], preferred_element_type=jnp.float32)
        kept = jnp.where(covered, placed, whole[:, cols].astype(jnp.float32))
        state_ref[:, cols] = kept.astype(jnp.bfloat16)

    settle(0)
    state_copy(1, True).wait_recv()
    settle(3)
    state_copy(3, True).wait_recv()
    settle(1)
    for kind in (4, 5):
        state_copy(kind, True).wait_recv()
    settle(2)
    for kind in range(6):
        state_copy(kind, False).wait_send()


def encode(patches, vis_gain, vis_bias, text, mask, own, place, small, proj):
    rows, width = patches.shape
    tiles = rows // PATCH
    block = text.shape[1] // 4
    length = text.shape[0] * 4
    share = PATCH // 4
    dma = pltpu.SemaphoreType.DMA
    vmem = pl.BlockSpec(memory_space=pltpu.VMEM)
    bf16 = jnp.bfloat16
    return pl.pallas_call(
        vision_kernel,
        out_shape=(
            jax.ShapeDtypeStruct((length, 4 * block), bf16),
            jax.ShapeDtypeStruct(mask.shape, jnp.float32),
        ),
        in_specs=[vmem] * 9,
        out_specs=(vmem, vmem),
        scratch_shapes=[
            pltpu.VMEM((small.shape[0] * 32, small.shape[1]), bf16),
            pltpu.VMEM((proj.shape[0] * 32, proj.shape[1]), bf16),
            pltpu.VMEM((rows, 3 * width // 4), jnp.float32),
            pltpu.VMEM((rows, width // 4), bf16),
            pltpu.VMEM((2, tiles, PATCH, width), bf16),
            pltpu.VMEM((2, tiles, 3, share, width), bf16),
            pltpu.VMEM((tiles, share, width), bf16),
            pltpu.VMEM((tiles, PATCH, width), bf16),
            pltpu.VMEM((tiles * POOL, 4 * width), bf16),
            pltpu.VMEM((4 * POOL, block), bf16),
            pltpu.VMEM((4 * POOL, block), bf16),
            pltpu.VMEM((4 * POOL, 4 * block), bf16),
            pltpu.VMEM((4, 4, 8, 128), jnp.float32),
            dma((2, 31)),
            dma((2, 31)),
            dma((4, tiles, 3)),
            dma((4, tiles, 3)),
            dma((3,)),
            dma((3,)),
            dma((6,)),
            dma((6,)),
            dma((4, 3)),
            dma((4, 3)),
            dma((2,)),
            pltpu.VMEM((length, 4 * block), bf16),
            dma((6,)),
            dma((6,)),
        ],
        compiler_params=pltpu.CompilerParams(
            collective_id=1, has_side_effects=True, vmem_limit_bytes=56 * 1024 * 1024
        ),
    )(patches, vis_gain, vis_bias, text, mask, own, place, small, proj)


def decoder_kernel(
    seg_col,
    seg_row,
    cos_ref,
    sin_ref,
    s0_ref,
    w_any,
    out_ref,
    xbuf,
    mbuf,
    wjb,
    wob,
    acc,
    ssq,
    kb,
    vb,
    bias,
    fin,
    hid,
    xs,
    xr,
    ms,
    mr,
    js,
    os,
    fs,
    fr,
    rs,
):
    parts = 4
    layers = 4
    copies = w_any.shape[0] // layers
    length = s0_ref.shape[0]
    block = s0_ref.shape[1] // parts
    half = length // 2
    joined = wjb.shape[2]
    query_width = wob.shape[1] // parts
    heads = query_width // HD
    depth = w_any.shape[1]
    col_share = wob.shape[2] // copies
    token_share = length // parts
    me = lax.axis_index("mp")
    right, opposite, left = (lax.rem(me + step, parts) for step in (1, 2, 3))

    def joined_copy(layer, par, d):
        return pltpu.make_async_copy(
            w_any.at[layer * copies + d, :, pl.ds(0, joined)],
            wjb.at[par, pl.ds(pl.multiple_of(d * depth, depth), depth), :],
            js.at[par, d],
        )

    def weight_copies(layer, par):
        found = [joined_copy(layer, par, d) for d in range(copies)]
        for d in range(copies):
            for part in range(parts):
                found.append(
                    pltpu.make_async_copy(
                        w_any.at[
                            layer * copies + d, :, pl.ds(joined + part * col_share, col_share)
                        ],
                        wob.at[par, pl.ds(part * depth, depth), pl.ds(d * col_share, col_share)],
                        os.at[par, d * parts + part],
                    )
                )
        return found[:copies], found[copies:]

    def piece(buf, width, sends, recvs, par, h, kind, source, half_at, target):
        cols = pl.ds(pl.multiple_of(source * width + half_at * (width // 2), width // 2), width // 2)
        ref = buf.at[par, pl.ds(h * half, half), cols]
        return pltpu.make_async_remote_copy(
            src_ref=ref,
            dst_ref=ref,
            send_sem=sends.at[par, h, kind],
            recv_sem=recvs.at[par, h, kind],
            device_id={"mp": target},
            device_id_type=MESH,
        )

    def sent(kind, buf, width, sends, recvs, par, h):
        source, half_at, target = (
            (me, 0, right),
            (me, 1, right),
            (me, 1, left),
            (me, 0, left),
            (left, 0, right),
            (right, 1, left),
        )[kind]
        return piece(buf, width, sends, recvs, par, h, kind, source, half_at, target)

    def landed(kind, buf, width, sends, recvs, par, h):
        source, half_at = (
            (left, 0),
            (left, 1),
            (right, 1),
            (right, 0),
            (opposite, 0),
            (opposite, 1),
        )[kind]
        return piece(buf, width, sends, recvs, par, h, kind, source, half_at, right)

    x_args = (xbuf, block, xs, xr)
    m_args = (mbuf, query_width, ms, mr)

    def forward(args, par, h):
        landed(0, *args, par, h).wait_recv()
        sent(4, *args, par, h).start()
        landed(2, *args, par, h).wait_recv()
        sent(5, *args, par, h).start()

    def waits(args, par, h, kinds):
        for kind in kinds:
            landed(kind, *args, par, h).wait_recv()

    def wait_sends(args, par, h):
        for kind in range(6):
            sent(kind, *args, par, h).wait_send()

    def start_own(par, h):
        for kind in (0, 2, 1, 3):
            sent(kind, *x_args, par, h).start()

    first_joined, first_out = weight_copies(0, 0)
    for copy in first_joined + first_out:
        copy.start()
    barrier = pltpu.get_barrier_semaphore()
    for target in (right, opposite, left):
        pl.semaphore_signal(barrier, inc=1, device_id={"mp": target}, device_id_type=MESH)
    own_cols = pl.ds(pl.multiple_of(me * block, block), block)
    ready = pltpu.make_async_copy(s0_ref, xbuf.at[0], rs.at[0])
    ready.start()
    rows_at = lax.broadcasted_iota(jnp.int32, (length, length), 0)
    cols_at = lax.broadcasted_iota(jnp.int32, (length, length), 1)
    allowed = (seg_col[...] == seg_row[...]) & (cols_at <= rows_at)
    bias[...] = jnp.where(allowed, 0.0, BLOCKED)
    pl.semaphore_wait(barrier, 3)
    ready.wait()

    def project(par, h, layer):
        rows = pl.ds(h * half, half)

        def add(source, first):
            if h == 0:
                for at in range(copies // parts):
                    joined_copy(layer, par, source * (copies // parts) + at).wait()
            cols = pl.ds(pl.multiple_of(source * block, block), block)
            values = xbuf[par, rows, cols]
            product = jnp.dot(values, wjb[par, cols, :], preferred_element_type=jnp.float32)
            wide = values.astype(jnp.float32)
            wide = wide * wide
            power = wide[:, :HD]
            for at in range(1, block // HD):
                power = power + wide[:, at * HD : (at + 1) * HD]
            if first:
                acc[:, :joined] = product
                ssq[...] = power
            else:
                acc[:, :joined] += product
                ssq[...] += power

        def arrive(step):
            @pl.when(layer > 0)
            def _():
                step()

        add(me, True)
        if h == 1:
            arrive(lambda: forward(x_args, par, h))
        arrive(lambda: waits(x_args, par, h, (1,)))
        add(left, False)
        arrive(lambda: waits(x_args, par, h, (3,)))
        add(right, False)
        if h == 1:
            forward(m_args, par, 0)
        arrive(lambda: waits(x_args, par, h, (4, 5)))
        add(opposite, False)

    def attend(par, h):
        rows = pl.ds(h * half, half)
        keys = half * (h + 1)
        power = jnp.sum(ssq[...], axis=1, keepdims=True) * (1.0 / (parts * block))
        scale = lax.rsqrt(power + EPS)
        cosine = cos_ref[rows, :] * scale
        sinus = sin_ref[rows, :] * scale

        def turned(at):
            values = acc[:, at * HD : (at + 1) * HD]
            return values * cosine + pltpu.roll(values, HD // 2, 1) * sinus

        kb[rows, :] = turned(heads).astype(jnp.bfloat16)
        vb[rows, :] = (acc[:, (heads + 1) * HD : (heads + 2) * HD] * scale).astype(jnp.bfloat16)
        for head in range(heads):
            query = (turned(head) * HD ** (-0.5)).astype(jnp.bfloat16)
            scores = lax.dot_general(
                query,
                kb[:keys, :],
                (((1,), (1,)), ((), ())),
                preferred_element_type=jnp.float32,
            )
            scores = scores + bias[rows, :keys]
            top = jnp.max(scores, axis=1, keepdims=True)
            probs = jnp.exp(scores - top)
            total = jnp.sum(probs, axis=1, keepdims=True)
            mixed = jnp.dot(
                probs.astype(jnp.bfloat16), vb[:keys, :], preferred_element_type=jnp.float32
            )
            cols = pl.ds(pl.multiple_of(me * query_width + head * HD, HD), HD)
            mbuf[par, rows, cols] = (mixed / total).astype(jnp.bfloat16)
            if head == heads // 2 - 1:
                sent(0, *m_args, par, h).start()
                sent(3, *m_args, par, h).start()
        sent(2, *m_args, par, h).start()
        sent(1, *m_args, par, h).start()

    def shared(target, source):
        return pltpu.make_async_remote_copy(
            src_ref=fin.at[pl.ds(target * token_share, token_share), :],
            dst_ref=hid.at[:, pl.ds(pl.multiple_of(source * block, block), block)],
            send_sem=fs.at[target],
            recv_sem=fr.at[source],
            device_id={"mp": target},
            device_id_type=MESH,
        )

    def leave(par, h, layer):
        rows = pl.ds(h * half, half)

        def term(source):
            cols = pl.ds(pl.multiple_of(source * query_width, query_width), query_width)
            return jnp.dot(
                mbuf[par, rows, cols], wob[par, cols, :], preferred_element_type=jnp.float32
            )

        acc[...] = xbuf[par, rows, own_cols].astype(jnp.float32) + term(me)
        waits(m_args, par, h, (1,))
        acc[...] += term(left)
        waits(m_args, par, h, (3,))
        acc[...] += term(right)
        waits(m_args, par, h, (4, 5))

        @pl.when(layer > 0)
        def _():
            wait_sends(x_args, par, h)

        result = (acc[...] + term(opposite)).astype(jnp.bfloat16)
        if h == 0:
            forward(m_args, par, 1)

        @pl.when(layer < layers - 1)
        def _():
            xbuf[1 - par, rows, own_cols] = result
            if h == 1:
                forward(x_args, 1 - par, 0)
            start_own(1 - par, h)

        @pl.when(layer == layers - 1)
        def _():
            fin[rows, :] = result
            for target in (2 * h, 2 * h + 1):

                @pl.when(target != me)
                def _():
                    shared(target, me).start()

                @pl.when(target == me)
                def _():
                    hid[:, own_cols] = fin[target * token_share : (target + 1) * token_share, :]

    def one_layer(layer, carry):
        par = lax.rem(layer, 2)
        out_copies = weight_copies(layer, par)[1]
        for h in range(2):
            project(par, h, layer)
            if h == 0:

                @pl.when(layer < layers - 1)
                def _():
                    for copies_of in weight_copies(layer + 1, 1 - par):
                        for copy in copies_of:
                            copy.start()

            @pl.when(layer > 0)
            def _():
                wait_sends(m_args, 1 - par, h)

            attend(par, h)
        for copy in out_copies:
            copy.wait()
        for h in range(2):
            leave(par, h, layer)
        return carry

    lax.fori_loop(0, layers, one_layer, 0)
    last = (layers - 1) % 2

    for h in range(2):
        wait_sends(m_args, last, h)
    for target in range(parts):

        @pl.when(target != me)
        def _():
            shared(target, me).wait_send()
            shared(target, target).wait_recv()

    out_ref[...] = hid[...]


def decode(state, segment_ids, weights):
    parts = lax.axis_size("mp")
    length, block = state.shape[0], state.shape[1] // parts
    copies = lax.axis_size(DP)
    depth = weights.shape[1]
    joined = weights.shape[2] - parts * (block // copies)
    cosine, sinus = rope_tables(length)
    dma = pltpu.SemaphoreType.DMA
    vmem = pl.BlockSpec(memory_space=pltpu.VMEM)
    return pl.pallas_call(
        decoder_kernel,
        out_shape=jax.ShapeDtypeStruct((length // parts, parts * block), jnp.bfloat16),
        in_specs=[vmem] * 4 + [pl.BlockSpec(memory_space=pl.ANY)] * 2,
        out_specs=vmem,
        scratch_shapes=[
            pltpu.VMEM((2, length, parts * block), jnp.bfloat16),
            pltpu.VMEM((2, length, parts * depth), jnp.bfloat16),
            pltpu.VMEM((2, copies * depth, joined), jnp.bfloat16),
            pltpu.VMEM((2, parts * depth, block), jnp.bfloat16),
            pltpu.VMEM((length // 2, block), jnp.float32),
            pltpu.VMEM((length // 2, HD), jnp.float32),
            pltpu.VMEM((length, HD), jnp.bfloat16),
            pltpu.VMEM((length, HD), jnp.bfloat16),
            pltpu.VMEM((length, length), jnp.float32),
            pltpu.VMEM((length, block), jnp.bfloat16),
            pltpu.VMEM((length // parts, parts * block), jnp.bfloat16),
            dma((2, 2, 6)),
            dma((2, 2, 6)),
            dma((2, 2, 6)),
            dma((2, 2, 6)),
            dma((2, copies)),
            dma((2, copies * parts)),
            dma((4,)),
            dma((4,)),
            dma((1,)),
        ],
        compiler_params=pltpu.CompilerParams(
            collective_id=0, has_side_effects=True, vmem_limit_bytes=60 * 1024 * 1024
        ),
    )(segment_ids[:, None], segment_ids[None, :], cosine, sinus, state, weights)


def shards(
    text,
    patches,
    segments,
    loss_mask,
    tile_batch,
    tile_offset,
    attn_gain,
    w_query,
    w_kv,
    w_out,
    vis_gain,
    vis_bias,
    v_qkv,
    v_out,
    v_up,
    v_down,
    v_proj,
):
    section_at = lax.axis_index("section")
    parts = lax.axis_size("mp")
    copies = lax.axis_size(DP)
    copy_at = lax.axis_index(DP)
    model_width = w_query.shape[1]
    row_share = model_width // copies
    pick = lambda array: lax.dynamic_slice_in_dim(array, copy_at * row_share, row_share, 0)
    own_rows = jnp.concatenate([pick(w_query[0]), pick(w_kv[0, 0]), pick(w_kv[0, 1])], axis=1)
    own_gain = lax.dynamic_slice_in_dim(attn_gain[0], copy_at * row_share, row_share, 0)
    own_rows = (own_rows.astype(jnp.float32) * own_gain[:, None]).astype(jnp.bfloat16)
    block_width = model_width // parts
    col_share = block_width // copies
    own_out = [
        lax.dynamic_slice_in_dim(w_out[0], part * block_width + copy_at * col_share, col_share, 1)
        for part in range(parts)
    ]
    own_out = lax.all_to_all(
        jnp.stack(own_out), "mp", split_axis=0, concat_axis=0, tiled=True
    )
    own_out = jnp.concatenate([own_out[part] for part in range(parts)], axis=1)
    own = jnp.concatenate([own_rows, own_out], axis=1)
    own, v_out, v_down = lax.optimization_barrier((own, v_out, v_down))
    small = jnp.concatenate([v_qkv[0], v_qkv[1], v_qkv[2], v_out.T, v_up, v_down.T], axis=1)
    sections = lax.axis_size("section")
    batch_all = tile_batch[0].reshape(sections, -1)
    offset_all = tile_offset[0].reshape(sections, -1)
    own_batch = lax.dynamic_slice_in_dim(batch_all, section_at, 1, 0)
    own_batch = jnp.repeat(own_batch, POOL, axis=1)
    starts = jnp.max(jnp.where(batch_all == section_at, offset_all, -POOL), axis=1)
    place = jnp.repeat(starts, POOL) + jnp.tile(jnp.arange(POOL, dtype=jnp.int32), sections)
    weights = lax.all_gather(own, SECTION_DP)
    state, token_weight = encode(
        patches,
        vis_gain,
        vis_bias,
        text[0],
        loss_mask,
        own_batch,
        place[None, :],
        small,
        v_proj,
    )
    hidden = decode(state, segments[0, 0], weights)
    return (hidden[None], token_weight)


def solution(mesh):
    split = Mesh(
        mesh.devices.reshape(mesh.shape["section"], 4, 2, mesh.shape["mp"]),
        ("section", "dp_0", "dp_1", "mp"),
    )
    return jax.shard_map(
        shards,
        mesh=split,
        in_specs=(
            P("section", DP_MP, None),
            P(SECTION_DP, None),
            P("section", DP, None),
            P("section", DP_MP),
            P(DP, None),
            P(DP, None),
            P("section", None),
            P("section", None, "mp"),
            P("section", None, None, "mp"),
            P("section", "mp", None),
            P(),
            P(),
            P(None, SECTION_DP, "mp"),
            P("mp", SECTION_DP),
            P(SECTION_DP, "mp"),
            P("mp", SECTION_DP),
            P(SECTION_DP, "mp"),
        ),
        out_specs=(P("section", DP_MP, None), P("section", DP_MP)),
        check_vma=False,
    )
```
